32 devices in a mesh: dp: 2 (over x), mp: 16 (over z, y, core).
Axes of the slice: x: 2, y: 2, z: 4, core: 2. Of those that a mesh axis runs over, the one named last changes fastest.
Arguments:
- grad_parts: bfloat16 [2, 16, 1, 512, 512], P('dp', 'mp'), may hold values from -0.1875 to 0.1875
- factors: float32 [16, 2, 512, 512], P('mp', 'dp'), may hold values from -1 to 8, as said below
- root_prev: bfloat16 [16, 2, 512, 512], P(None, 'dp', 'mp'), may hold values from -1 to 2, as said below
- plan: int32 [2, 16], P('dp'), may hold values from 0 to 16, as said below
Outputs:
- new_factors: float32 [16, 2, 512, 512], P('mp', 'dp')
- new_roots: bfloat16 [16, 2, 512, 512], P(None, 'dp', 'mp')
The draws below stay inside these ranges and needn't reach their ends.
Inputs may be any that keep to these rules, and one draw needn't show every extreme that they name: In each row of plan no worker is named more than 3 times and one is named exactly 3 times; at least 8 entries of a row are below 16. `factors`: each factor is symmetric. `root_prev`: each root is symmetric.
All inputs are finite; a program needn't handle non-finite values.
Results may differ from the reference program's by a relative error of at most 0.0055.
Values may be sent and summed in bfloat16 or wider, within the bound.
A program may use at most 64 MiB of HBM per device.

```python
import jax
import jax.numpy as jnp
from jax import lax

BS = 512
CAP = 3
HALF = 1
N_DP = 2
N_MP = 16


def spectrum(key):
    upper_end = 4.0
    uniform_draw = jax.random.uniform(jax.random.fold_in(key, 11), (N_MP, N_DP, BS), jnp.float32)
    return 0.5 * jnp.exp(uniform_draw * jnp.log(upper_end / 0.5))


def symmetric(key):
    noise = jax.random.normal(key, (N_MP, N_DP, BS, BS), jnp.float32)
    return (noise + jnp.swapaxes(noise, -1, -2)) * 0.5 ** 0.5


def draw_factors(key, part):
    diagonal_vals = spectrum(key)
    identity = jnp.eye(BS, dtype=jnp.float32)
    outer_scale = jnp.sqrt(diagonal_vals[..., :, None] * diagonal_vals[..., None, :])
    spread = symmetric(jax.random.fold_in(key, 12)) * (0.25 / BS ** 0.5)
    result = outer_scale * spread * (1.0 - identity) + identity * diagonal_vals[..., None, :]
    return result.astype(jnp.float32)


def draw_root_prev(key, part):
    diagonal_vals = spectrum(key)
    identity = jnp.eye(BS, dtype=jnp.float32)
    scaling = diagonal_vals ** (-0.125)
    spread = symmetric(jax.random.fold_in(key, 13)) * (0.2 / BS ** 0.5)
    inner = identity + spread * (1.0 - identity)
    result = scaling[..., :, None] * inner * scaling[..., None, :]
    return result.astype(jnp.bfloat16)


def plan_row(key):
    refreshed = jax.random.randint(jax.random.fold_in(key, 1), (), N_MP // 2, N_MP + 1)
    rank_of = jax.random.permutation(jax.random.fold_in(key, 2), N_MP)
    shuffled = jax.random.permutation(jax.random.fold_in(key, 3), N_MP)
    busiest = shuffled[0]
    remaining = shuffled[1:]
    workers = jnp.concatenate([jnp.full((CAP,), busiest), jnp.full((2,), remaining[0]), remaining[1:]])
    chosen = workers[rank_of]
    return jnp.where(rank_of < refreshed, chosen, N_MP).astype(jnp.int32)


def draw_plan(key, part):
    row_keys = jax.random.split(key, N_DP)
    return jax.vmap(plan_row)(row_keys)


def shard_levels(rng, extent, pieces, smallest, largest):
    level, own = 1.0, jax.random.fold_in(rng, 6)
    for axis_at, shards_of in pieces:
        heights = jnp.exp(jax.random.uniform(jax.random.fold_in(own, axis_at), (shards_of,), jnp.float32, smallest / len(pieces), largest / len(pieces)))
        level = level * jnp.repeat(heights, extent[axis_at] // shards_of).reshape([-1 if axis == axis_at else 1 for axis in range(len(extent))])
    return level


def normal_values(rng, dims, deviation, bound, pieces=(), kind=jnp.bfloat16):
    level = shard_levels(rng, dims, pieces, -0.22, 0.18) if pieces else 1.0
    values = jax.random.normal(rng, dims, jnp.float32) * deviation * level
    return jnp.minimum(jnp.maximum(values, -bound), bound).astype(kind)


def setup_inputs(seed: int = 0) -> dict:
    streams_of = jax.random.split(jax.random.key(seed), 5)
    grad_parts = normal_values(streams_of[0], (N_DP, N_MP, HALF, BS, BS), (BS * N_DP) ** -0.5, 0.1875, ((0, 2), (1, 16)))
    factors = draw_factors(jax.random.fold_in(streams_of[4], 71), 0)
    root_prev = draw_root_prev(jax.random.fold_in(streams_of[4], 71), 0)
    plan = draw_plan(jax.random.fold_in(streams_of[4], 71), 0)
    return dict(grad_parts=grad_parts, factors=factors, root_prev=root_prev, plan=plan)


keep_rate = 0.8


def newton(initial, factor):
    identity = jnp.eye(factor.shape[-1], dtype=jnp.float32)
    square = jnp.einsum("sij,sjk->sik", initial, initial, preferred_element_type=jnp.float32)
    fourth = jnp.einsum("sij,sjk->sik", square, square, precision=lax.Precision.HIGHEST)
    coupled = jnp.einsum("sij,sjk->sik", fourth, factor, precision=lax.Precision.HIGHEST)
    update = (5.0 * identity - coupled) * 0.25
    return jnp.einsum("sij,sjk->sik", initial.astype(jnp.float32), update, precision=lax.Precision.HIGHEST)


def reference(grad_parts, factors, root_prev, plan):
    def per_owner(owner):
        partial_grads = lax.dynamic_index_in_dim(grad_parts, owner, 1, keepdims=False)
        summed = jnp.sum(partial_grads.astype(jnp.float32), axis=0)
        left = jnp.einsum("kij,klj->kil", summed, summed, precision=lax.Precision.HIGHEST)
        right = jnp.einsum("kji,kjl->kil", summed, summed, precision=lax.Precision.HIGHEST)
        grams = jnp.stack([left, right], axis=1).reshape(N_DP, BS, BS)
        old_factor = lax.dynamic_index_in_dim(factors, owner, 0, keepdims=False)
        fresh_factor = keep_rate * old_factor + (1.0 - keep_rate) * grams
        previous = lax.dynamic_index_in_dim(root_prev, owner, 0, keepdims=False)
        refined = newton(previous, fresh_factor).astype(jnp.bfloat16)
        owner_plan = lax.dynamic_index_in_dim(plan, owner, 1, keepdims=False)
        roots = jnp.where(owner_plan[:, None, None] < N_MP, refined, previous)
        return fresh_factor, roots

    new_factors, new_roots = lax.map(per_owner, jnp.arange(N_MP, dtype=jnp.int32))
    return new_factors, new_roots
```

```python
import functools

import jax
import jax.numpy as jnp
from jax import lax
from jax.experimental import pallas as pl
from jax.experimental.pallas import tpu as pltpu
from jax.sharding import PartitionSpec as P

keep_rate = 0.8
CHUNKS = 8
GROUP = 2
TURN = 5
MESH = pl.DeviceIdType.MESH
F32 = jnp.float32
BF16 = jnp.bfloat16


def mul(a, b):
    return jnp.dot(a, b, preferred_element_type=F32)


def scope(name):
    return jax.named_scope(name)


def kernel(
    n_dp, n_mp, blocks, row,
    plan, grad, fac, root, fresh, fac_out, plan_s,
    own_g, in_g, fac_v, root_v, pieces, full_x, rest, fifth, summed, gram_v, out_v,
    load_sem, grad_send, grad_recv, root_send, root_recv, out_send, out_recv, turn, above, below,
):
    d = lax.axis_index("dp")
    me = lax.axis_index("mp")
    bs = fac.shape[-1]
    half = n_mp // 2
    hb = bs // 2
    part = bs // CHUNKS
    wide = part * GROUP
    groups = CHUNKS // GROUP
    levels = n_mp // row
    level = me // row
    at = me % row
    side = me // half
    away = 1 - side
    near_cols = pl.ds(pl.multiple_of(side * hb, hb), hb)
    far_cols = pl.ds(pl.multiple_of(away * hb, hb), hb)
    far_first = pl.ds(pl.multiple_of(away * hb, hb), hb // 2)
    far_second = pl.ds(pl.multiple_of(away * hb + hb // 2, hb // 2), hb // 2)
    near_pieces = pl.ds(side * half, half)
    far_pieces = pl.ds(away * half, half)
    lead = me % 2 == 0
    has_above = level < levels - 1
    has_below = level > 0

    loads = [
        pltpu.make_async_copy(grad, own_g, load_sem.at[0]),
        pltpu.make_async_copy(root, root_v, load_sem.at[1]),
        pltpu.make_async_copy(root.at[me], pieces.at[me], load_sem.at[2]),
        pltpu.make_async_copy(fac, fac_v, load_sem.at[3]),
        pltpu.make_async_copy(plan, plan_s, load_sem.at[4]),
    ]

    def signal(sem, dp, mp):
        pl.semaphore_signal(sem, inc=1, device_id=(dp, mp), device_id_type=MESH)

    with scope("BARRIER"):
        barrier = pltpu.get_barrier_semaphore()
        for i in range(1, n_dp):
            signal(barrier, (d + i) % n_dp, me)
        for i in range(1, row):
            signal(barrier, d, level * row + (at + i) % row)

        @pl.when(has_below)
        def _():
            signal(barrier, d, me - row)

        @pl.when(has_above)
        def _():
            signal(barrier, d, me + row)

        for load in loads:
            load.start()
        pl.semaphore_wait(barrier, n_dp - 1 + row - 1 + has_below.astype(jnp.int32) + has_above.astype(jnp.int32))

        @pl.when(has_below)
        def _():
            signal(above.at[1], d, me - row)

        @pl.when(has_above)
        def _():
            signal(below.at[1], d, me + row)

        loads[0].wait()

    def grad_copy(i, c):
        other = (d + i) % n_dp
        rows = pl.ds(c * part, part)
        return pltpu.make_async_remote_copy(
            src_ref=own_g.at[other * blocks // n_dp, rows], dst_ref=in_g.at[i - 1, rows],
            send_sem=grad_send.at[i - 1, c], recv_sem=grad_recv.at[i - 1, c],
            device_id=(other, me), device_id_type=MESH,
        )

    grad_copies = [grad_copy(i, c) for c in range(CHUNKS) for i in range(1, n_dp)]

    @pl.when(lead)
    def _():
        for copy in grad_copies:
            copy.start()

    def root_far(src, dst, peer, slot, origin, act):
        base = origin // half * hb
        upper = origin % half < half // 2

        def copy(start, size):
            cols = pl.ds(pl.multiple_of(start, hb // 2), size)
            return pltpu.make_async_remote_copy(
                src_ref=root_v.at[src, :, cols], dst_ref=pieces.at[dst, :, cols],
                send_sem=root_send.at[peer], recv_sem=root_recv.at[slot],
                device_id=(d, peer), device_id_type=MESH,
            )

        @pl.when(upper)
        def _():
            act(copy(base, hb))

        @pl.when(jnp.logical_not(upper))
        def _():
            act(copy(base + hb // 2, hb // 2))

    def root_near(src, dst, peer, slot):
        return pltpu.make_async_remote_copy(
            src_ref=root_v.at[src], dst_ref=pieces.at[dst],
            send_sem=root_send.at[peer], recv_sem=root_recv.at[slot],
            device_id=(d, peer), device_id_type=MESH,
        )

    def send_roots(to, parity):
        for j in range(row // 2):
            t = to * row + (at // 2 * 2 + 2 * j) % row + parity
            close = t // half == side

            @pl.when(jnp.logical_not(close))
            def _():
                root_far(t, me, t, me, me, lambda copy: copy.start())

            @pl.when(jnp.logical_and(close, t != me))
            def _():
                root_near(t, me, t, me).start()

    def each_level(parity, meet):
        for k in range(1, levels):
            @pl.when(level + k < levels)
            def _():
                if meet:
                    pl.semaphore_wait(above.at[k], 1)
                    if k + 1 < levels:
                        @pl.when(has_below)
                        def _():
                            signal(above.at[k + 1], d, me - row)
                send_roots(level + k, parity)

            @pl.when(level >= k)
            def _():
                if meet:
                    pl.semaphore_wait(below.at[k], 1)
                    if k + 1 < levels:
                        @pl.when(has_above)
                        def _():
                            signal(below.at[k + 1], d, me + row)
                send_roots(level - k, parity)

        send_roots(level, parity)

    with scope("ROOTSEND"):
        loads[1].wait()
        each_level(0, True)

    with scope("TURN"):
        early = TURN * (n_dp - 1)

        @pl.when(lead)
        def _():
            for copy in grad_copies[:early]:
                copy.wait_send()
            signal(turn, d, me + 1)

        @pl.when(jnp.logical_not(lead))
        def _():
            pl.semaphore_wait(turn, 1)
            for copy in grad_copies:
                copy.start()

        each_level(1, False)

    def take_grad(c):
        rows = pl.ds(c * wide, wide)
        for j in range(GROUP):
            for i in range(1, n_dp):
                grad_copy(i, c * GROUP + j).wait_recv()
        total = own_g[d * blocks // n_dp, rows].astype(F32)
        for i in range(1, n_dp):
            total += in_g[i - 1, rows].astype(F32)
        s = total.astype(BF16)

        @pl.when(d % 2 == 0)
        def _():
            summed[rows, :] = s
            so_far = pl.ds(0, (c + 1) * wide)
            gram_v[rows, so_far] = lax.dot_general(s, summed[so_far, :], (((1,), (1,)), ((), ())), preferred_element_type=F32)
            if c:
                before = pl.ds(0, c * wide)
                gram_v[before, rows] = lax.dot_general(summed[before, :], s, (((1,), (1,)), ((), ())), preferred_element_type=F32)

        @pl.when(d % 2 == 1)
        def _():
            term = lax.dot_general(s, s, (((0,), (0,)), ((), ())), preferred_element_type=F32)
            gram_v[...] = term if c == 0 else gram_v[...] + term

    with scope("EARLYGRAD"):
        @pl.when(lead)
        def _():
            for c in range(groups - 1):
                take_grad(c)

    with scope("ROOTRECV"):
        loads[2].wait()
        loads[3].wait()

        @pl.loop(0, half)
        def _(i):
            s = away * half + i
            root_far(s, s, s, s, s, lambda copy: copy.wait_recv())

        @pl.loop(1, half)
        def _(i):
            s = side * half + (me + i) % half
            root_near(s, s, s, s).wait_recv()

    with scope("ASSEMBLE"):
        near_rows = pieces[near_pieces].astype(F32).reshape(hb, bs).astype(BF16)
        full_x[near_cols, :] = near_rows
        full_x[far_cols, far_cols] = pieces[far_pieces, :, far_cols].astype(F32).reshape(hb, hb).astype(BF16)
        full_x[far_second, far_first] = full_x[far_first, far_second].astype(F32).T.astype(BF16)
        full_x[far_cols, near_cols] = full_x[near_cols, far_cols].astype(F32).T.astype(BF16)

    with scope("CHAIN"):
        x = full_x[...]
        square = mul(x, x).astype(BF16)
        fourth = mul(square, square).astype(BF16)
        fifth[...] = mul(x, fourth).astype(BF16)
        rest[...] = 1.25 * x.astype(F32) - (0.25 * keep_rate) * mul(fifth[...], fac_v[...].astype(BF16))

    with scope("GRADS"):
        @pl.when(jnp.logical_not(lead))
        def _():
            for c in range(groups - 1):
                take_grad(c)
    with scope("GRADLAST"):
        take_grad(groups - 1)

    with scope("GRAMH"):
        gram_h = gram_v[...].astype(BF16)
        loads[4].wait()
        kept = plan_s[0, me] >= n_mp

    def out_copy(src, dst, peer, slot):
        return pltpu.make_async_remote_copy(
            src_ref=out_v.at[src], dst_ref=fresh.at[dst],
            send_sem=out_send.at[peer], recv_sem=out_recv.at[slot],
            device_id=(d, peer), device_id_type=MESH,
        )

    def refine(rows, to):
        refined = rest[rows, :] - (0.25 * (1.0 - keep_rate)) * mul(fifth[rows, :], gram_h)
        refined = jnp.where(kept, full_x[rows, :].astype(F32), refined)
        out_v[to] = refined.reshape(half, bs // n_mp, bs).astype(BF16)

    def send_out(t):
        out_copy(t, me, t, me).start()

    with scope("REF1"):
        refine(far_cols, far_pieces)

        @pl.loop(0, half // row)
        def _(k):
            for j in range(row):
                send_out(away * half + k * row + (at + j) % row)

    with scope("REF2"):
        refine(near_cols, near_pieces)

        @pl.loop(1, half)
        def _(i):
            send_out(side * half + (me + i) % half)

    with scope("FACOUT"):
        own_out = pltpu.make_async_copy(out_v.at[me], fresh.at[me], load_sem.at[0])
        own_out.start()
        fac_out[...] = keep_rate * fac_v[...] + (1.0 - keep_rate) * gram_v[...]

    with scope("SENDS"):
        @pl.when(lead)
        def _():
            for copy in grad_copies[early:]:
                copy.wait_send()

        @pl.when(jnp.logical_not(lead))
        def _():
            for copy in grad_copies:
                copy.wait_send()

        @pl.loop(0, half)
        def _(i):
            t = away * half + i
            root_far(t, me, t, me, me, lambda copy: copy.wait_send())

        @pl.loop(1, half)
        def _(i):
            t = side * half + (me + i) % half
            root_near(t, me, t, me).wait_send()

        @pl.loop(1, n_mp)
        def _(i):
            s = (me + i) % n_mp
            out_copy(s, s, s, s).wait_send()

        own_out.wait()

    with scope("RECVNEAR"):
        @pl.loop(1, half)
        def _(i):
            s = side * half + (me + i) % half
            out_copy(s, s, s, s).wait_recv()

    with scope("RECVFAR"):
        @pl.loop(0, half)
        def _(i):
            s = away * half + i
            out_copy(s, s, s, s).wait_recv()


def write_out(fac_v, fresh_v, fac_out, fresh_out, sem):
    n = 4
    copies = []
    for i in range(n):
        a = pl.ds(i * (fac_v.shape[0] // n), fac_v.shape[0] // n)
        b = pl.ds(i * (fresh_v.shape[0] // n), fresh_v.shape[0] // n)
        copies.append(pltpu.make_async_copy(fac_v.at[a], fac_out.at[a], sem.at[2 * i]))
        copies.append(pltpu.make_async_copy(fresh_v.at[b], fresh_out.at[b], sem.at[2 * i + 1]))
    for copy in copies:
        copy.start()
    for copy in copies:
        copy.wait()


def level_size(n_mp):
    size = 1
    while size * size < n_mp:
        size *= 2
    return size


def local(n_dp, n_mp, grad_parts, factors, root_prev, plan):
    blocks, bs = grad_parts.shape[2], factors.shape[-1]
    rows = bs // n_mp
    row = level_size(n_mp)
    grads = grad_parts.reshape(blocks, bs, bs)
    old = root_prev.reshape(n_mp, rows, bs)
    fresh, new_factor = pl.pallas_call(
        functools.partial(kernel, n_dp, n_mp, blocks, row),
        out_shape=(
            pltpu.VMEM((n_mp, rows, bs), BF16),
            pltpu.VMEM((bs, bs), F32),
        ),
        in_specs=[pl.BlockSpec(memory_space=pl.ANY)] * 4,
        out_specs=(pl.BlockSpec(memory_space=pltpu.VMEM),) * 2,
        scratch_shapes=[
            pltpu.SMEM(plan.shape, plan.dtype),
            pltpu.VMEM((blocks, bs, bs), BF16),
            pltpu.VMEM((n_dp - 1, bs, bs), BF16),
            pltpu.VMEM((bs, bs), F32),
            pltpu.VMEM((n_mp, rows, bs), BF16),
            pltpu.VMEM((n_mp, rows, bs), BF16),
            pltpu.VMEM((bs, bs), BF16),
            pltpu.VMEM((bs, bs), F32),
            pltpu.VMEM((bs, bs), BF16),
            pltpu.VMEM((bs, bs), BF16),
            pltpu.VMEM((bs, bs), F32),
            pltpu.VMEM((n_mp, rows, bs), BF16),
            pltpu.SemaphoreType.DMA((5,)),
            pltpu.SemaphoreType.DMA((n_dp - 1, CHUNKS)),
            pltpu.SemaphoreType.DMA((n_dp - 1, CHUNKS)),
            pltpu.SemaphoreType.DMA((n_mp,)),
            pltpu.SemaphoreType.DMA((n_mp,)),
            pltpu.SemaphoreType.DMA((n_mp,)),
            pltpu.SemaphoreType.DMA((n_mp,)),
            pltpu.SemaphoreType.REGULAR,
            pltpu.SemaphoreType.REGULAR((n_mp // row,)),
            pltpu.SemaphoreType.REGULAR((n_mp // row,)),
        ],
        compiler_params=pltpu.CompilerParams(collective_id=0, has_side_effects=True),
        name="refresh",
    )(plan, grads, factors.reshape(bs, bs), old)
    new_factor, fresh = pl.pallas_call(
        write_out,
        out_shape=(
            jax.ShapeDtypeStruct((bs, bs), F32),
            jax.ShapeDtypeStruct((n_mp, rows, bs), BF16),
        ),
        in_specs=[pl.BlockSpec(memory_space=pl.ANY)] * 2,
        out_specs=(pl.BlockSpec(memory_space=pl.ANY),) * 2,
        scratch_shapes=[pltpu.SemaphoreType.DMA((8,))],
        compiler_params=pltpu.CompilerParams(vmem_limit_bytes=1 << 20),
        name="write_out",
    )(new_factor, fresh)
    return (new_factor[None, None], fresh.reshape(root_prev.shape))


def solution(mesh):
    return jax.shard_map(
        functools.partial(local, mesh.shape["dp"], mesh.shape["mp"]),
        mesh=mesh,
        in_specs=(
            P("dp", "mp", None, None, None),
            P("mp", "dp", None, None),
            P(None, "dp", "mp", None),
            P("dp", None),
        ),
        out_specs=(P("mp", "dp", None, None), P(None, "dp", "mp", None)),
        check_vma=False,
    )
```

```python
import functools

import jax
import jax.numpy as jnp
from jax import lax
from jax.experimental import pallas as pl
from jax.experimental.pallas import tpu as pltpu
from jax.sharding import PartitionSpec as P

keep_rate = 0.8
fresh_rate = 1.0 - keep_rate
GROUPS = 4
MESH = pl.DeviceIdType.MESH
F32 = jnp.float32
BF16 = jnp.bfloat16
scope = jax.named_scope


def mul(a, b, dims=(1, 0)):
    return lax.dot_general(a, b, (((dims[0],), (dims[1],)), ((), ())), preferred_element_type=F32)


def wait_bytes(ref, sem):
    pltpu.make_async_copy(ref, ref, sem).wait()


def kernel(
    n_dp, n_mp, blocks, row,
    plan, grad, fac, root, fresh, fac_out, plan_s,
    own_g, in_g, fac_v, pieces, full_x, rest, fifth, fac_b, summed, gram_b, out_v,
    load_sem, grad_send, grad_recv, gram_send, gram_recv, root_send, root_recv, out_send, out_recv, above,
):
    d = lax.axis_index("dp")
    me = lax.axis_index("mp")
    bs = fac.shape[-1]
    high = bs // n_mp
    half = n_mp // 2
    hb = bs // 2
    wide = bs // GROUPS
    levels = n_mp // row
    level = me // row
    at = me % row
    side = me // half
    away = 1 - side
    near_cols = pl.ds(pl.multiple_of(side * hb, hb), hb)
    far_cols = pl.ds(pl.multiple_of(away * hb, hb), hb)
    far_first = pl.ds(pl.multiple_of(away * hb, hb), hb // 2)
    far_second = pl.ds(pl.multiple_of(away * hb + hb // 2, hb // 2), hb // 2)
    near_pieces = pl.ds(side * half, half)
    far_pieces = pl.ds(away * half, half)
    parity = me % 2
    collects = d % 2 == parity
    partner = d + 1 - 2 * (d % 2)

    loads = [
        pltpu.make_async_copy(grad.at[d // 2], own_g, load_sem.at[0]),
        pltpu.make_async_copy(root.at[me], pieces.at[me], load_sem.at[1]),
        pltpu.make_async_copy(fac, fac_v, load_sem.at[2]),
        pltpu.make_async_copy(plan, plan_s, load_sem.at[3]),
    ]

    def signal(sem, dp, mp):
        pl.semaphore_signal(sem, inc=1, device_id=(dp, mp), device_id_type=MESH)

    def by_parity(act):
        @pl.when(parity == 0)
        def _():
            act(True)

        @pl.when(parity == 1)
        def _():
            act(False)

    with scope("BARRIER"):
        barrier = pltpu.get_barrier_semaphore()
        for i in range(1, n_dp):
            signal(barrier, (d + i) % n_dp, me)
        for i in range(1, row):
            signal(barrier, d, level * row + (at + i) % row)

        for k in range(1, levels):
            @pl.when(level + k < levels)
            def _():
                for i in range(row):
                    signal(barrier, d, (level + k) * row + (at + i) % row)

        for load in loads:
            load.start()
        pl.semaphore_wait(barrier, n_dp - 1 + row - 1 + level * row)

        for k in range(1, levels):
            @pl.when(level >= k)
            def _():
                signal(above.at[k], d, me - k * row)

    def strip(ref, c, by_cols):
        cut = pl.ds(c * wide, wide)
        return ref.at[:, cut] if by_cols else ref.at[cut, :]

    def send_grads(by_cols):
        for c in range(GROUPS):
            for k in range(blocks):
                to = 2 * k + parity

                @pl.when(to != d)
                def _():
                    pltpu.make_async_remote_copy(
                        src_ref=strip(grad.at[k], c, by_cols),
                        dst_ref=strip(in_g.at[(d - to + n_dp) % n_dp - 1], c, by_cols),
                        send_sem=grad_send.at[c // (GROUPS - 1)], recv_sem=grad_recv.at[c],
                        device_id=(to, me), device_id_type=MESH,
                    ).start()

    by_parity(send_grads)

    def root_far(t):
        base = side * hb
        upper = me % half < half // 2

        def copy(start, size):
            cols = pl.ds(pl.multiple_of(start, hb // 2), size)
            pltpu.make_async_remote_copy(
                src_ref=root.at[t, :, cols], dst_ref=pieces.at[me, :, cols],
                send_sem=root_send, recv_sem=root_recv, device_id=(d, t), device_id_type=MESH,
            ).start()

        @pl.when(upper)
        def _():
            copy(base, hb)

        @pl.when(jnp.logical_not(upper))
        def _():
            copy(base + hb // 2, hb // 2)

    def root_near(t):
        pltpu.make_async_remote_copy(
            src_ref=root.at[t], dst_ref=pieces.at[me],
            send_sem=root_send, recv_sem=root_recv, device_id=(d, t), device_id_type=MESH,
        ).start()

    def send_roots(to, odd):
        for j in range(row // 2):
            t = to * row + (at // 2 * 2 + 2 * j) % row + odd
            close = t // half == side

            @pl.when(jnp.logical_not(close))
            def _():
                root_far(t)

            @pl.when(jnp.logical_and(close, t != me))
            def _():
                root_near(t)

    def each_level(odd, meet):
        for k in reversed(range(1, levels)):
            @pl.when(level >= k)
            def _():
                send_roots(level - k, odd)

        send_roots(level, odd)

        for k in range(1, levels):
            @pl.when(level + k < levels)
            def _():
                if meet:
                    pl.semaphore_wait(above.at[k], 1)
                send_roots(level + k, odd)

    with scope("ROOTSEND"):
        each_level(d % 2, True)

    def take(c, by_cols):
        wait_bytes(in_g.at[:, :, pl.ds(c * wide, wide)] if by_cols else in_g.at[:, pl.ds(c * wide, wide), :], grad_recv.at[c])
        total = strip(own_g, c, by_cols)[...].astype(F32)
        for i in range(n_dp - 1):
            total += strip(in_g.at[i], c, by_cols)[...].astype(F32)
        strip(summed, c, by_cols)[...] = total.astype(BF16)

    def make_row(c, by_cols):
        new = strip(summed, c, by_cols)[...]
        so_far = pl.ds(0, (c + 1) * wide)
        product = mul(new, summed[:, so_far], (0, 0)) if by_cols else mul(new, summed[so_far, :], (1, 1))
        gram_b[pl.ds(c * wide, wide), so_far] = (fresh_rate * product).astype(BF16)

    def gram_row(c):
        part = gram_b.at[pl.ds(c * wide, wide), pl.ds(0, (c + 1) * wide)]
        return pltpu.make_async_remote_copy(
            src_ref=part, dst_ref=part, send_sem=gram_send.at[c], recv_sem=gram_recv.at[c],
            device_id=(partner, me), device_id_type=MESH,
        )

    early = GROUPS // 2
    loads[0].wait()

    with scope("EARLY"):
        @pl.when(collects)
        def _():
            def act(by_cols):
                for c in range(early):
                    take(c, by_cols)
                    make_row(c, by_cols)
                    if c == 0:
                        each_level(1 - d % 2, False)

            by_parity(act)

        @pl.when(jnp.logical_not(collects))
        def _():
            wait_bytes(in_g.at[pl.ds(0, blocks), pl.ds(0, bs - wide), :], grad_send.at[0])
            each_level(1 - d % 2, False)

    with scope("ROOTRECV"):
        loads[1].wait()
        loads[2].wait()
        wait_bytes(pieces.at[pl.ds(0, half - 1 + half * 3 // 8)], root_recv)

    loads[3].wait()
    kept = plan_s[0, me] >= n_mp
    x_rate = jnp.where(kept, 1.0, 1.25)
    step = jnp.where(kept, 0.0, 0.25)

    with scope("ASSEMBLE"):
        near_rows = pieces[near_pieces].astype(F32).reshape(hb, bs).astype(BF16)
        full_x[near_cols, :] = near_rows
        full_x[far_cols, far_cols] = pieces[far_pieces, :, far_cols].astype(F32).reshape(hb, hb).astype(BF16)
        full_x[far_second, far_first] = full_x[far_first, far_second].astype(F32).T.astype(BF16)
        full_x[far_cols, near_cols] = full_x[near_cols, far_cols].astype(F32).T.astype(BF16)

    with scope("CHAIN"):
        x = full_x[...]
        square = mul(x, x).astype(BF16)
        fourth = mul(square, square).astype(BF16)
        fifth[...] = (step * mul(x, fourth)).astype(BF16)

    def send_out(t):
        pltpu.make_async_remote_copy(
            src_ref=out_v.at[t], dst_ref=fresh.at[me],
            send_sem=out_send, recv_sem=out_recv, device_id=(d, t), device_id_type=MESH,
        ).start()

    def refine(first, count, base, factor):
        rows = pl.ds(pl.multiple_of(first * high, high), count * high)
        refined = base(rows) - mul(fifth[rows, :], factor[...])
        out_v[pl.ds(first, count)] = refined.reshape(count, high, bs).astype(BF16)

    def give_far(base, factor):
        for k in range(half // row):
            refine(away * half + k * row, row, base, factor)
            for j in range(row):
                send_out(away * half + k * row + j // 2 * 2 + (j + at) % 2)

    def give_near(base, factor):
        refine(side * half, half, base, factor)

        @pl.loop(1, half)
        def _(i):
            send_out(side * half + (me + i) % half)

    def part_x(rows):
        return x_rate * full_x[rows, :].astype(F32)

    @pl.when(collects)
    def _():
        def act(by_cols):
            dims = (1, 1) if by_cols else (0, 0)
            last = GROUPS - 1
            with scope("GRADS"):
                for c in range(early, last):
                    take(c, by_cols)
                    make_row(c, by_cols)
                for c in range(last):
                    gram_row(c).start()
                cut = pl.ds(0, last * wide)
                known = summed[:, cut] if by_cols else summed[cut, :]
                fac_out[...] = keep_rate * fac_v[...] + fresh_rate * mul(known, known, dims)
            with scope("GRADLAST"):
                take(last, by_cols)
                new = strip(summed, last, by_cols)[...]
                total = fac_out[...] + fresh_rate * mul(new, new, dims)
                fac_out[...] = total
                fac_b[...] = total.astype(BF16)
            with scope("GIVEFAR"):
                give_far(part_x, fac_b)
            with scope("ROWLAST"):
                make_row(last, by_cols)
                gram_row(last).start()
            with scope("GIVENEAR"):
                give_near(part_x, fac_b)
            for c in range(GROUPS):
                gram_row(c).wait_send()

        by_parity(act)

    @pl.when(jnp.logical_not(collects))
    def _():
        with scope("REST"):
            rest[...] = x_rate * full_x[...].astype(F32) - keep_rate * mul(fifth[...], fac_v[...].astype(BF16))
        for c in range(GROUPS):
            with scope("GRAMIN%d" % c):
                gram_row(c).wait_recv()
                if c:
                    rows = pl.ds(c * wide, wide)
                    before = pl.ds(0, c * wide)
                    gram_b[before, rows] = gram_b[rows, before].astype(F32).T.astype(BF16)
        with scope("GIVEFAR"):
            give_far(lambda rows: rest[rows, :], gram_b)
        with scope("GIVENEAR"):
            give_near(lambda rows: rest[rows, :], gram_b)
        with scope("FACOUT"):
            fac_out[...] = keep_rate * fac_v[...] + gram_b[...].astype(F32)
            wait_bytes(in_g.at[pl.ds(0, blocks), pl.ds(0, wide), :], grad_send.at[1])

    with scope("SENDS"):
        own_out = pltpu.make_async_copy(out_v.at[me], fresh.at[me], load_sem.at[0])
        own_out.start()
        if blocks > 1:
            @pl.when(collects)
            def _():
                wait_bytes(in_g.at[pl.ds(0, blocks - 1), pl.ds(0, bs - wide), :], grad_send.at[0])
                wait_bytes(in_g.at[pl.ds(0, blocks - 1), pl.ds(0, wide), :], grad_send.at[1])

        @pl.when(me % half < half // 2)
        def _():
            wait_bytes(pieces.at[pl.ds(0, half - 1 + half // 2)], root_send)

        @pl.when(me % half >= half // 2)
        def _():
            wait_bytes(pieces.at[pl.ds(0, half - 1 + half // 4)], root_send)

        own_out.wait()
        wait_bytes(out_v.at[pl.ds(0, n_mp - 1)], out_send)

    with scope("RECV"):
        wait_bytes(fresh.at[pl.ds(0, n_mp - 1)], out_recv)


def write_out(fac_v, fresh_v, fac_out, fresh_out, sem):
    n = 4
    copies = []
    for i in range(n):
        a = pl.ds(i * (fac_v.shape[0] // n), fac_v.shape[0] // n)
        b = pl.ds(i * (fresh_v.shape[0] // n), fresh_v.shape[0] // n)
        copies.append(pltpu.make_async_copy(fac_v.at[a], fac_out.at[a], sem.at[2 * i]))
        copies.append(pltpu.make_async_copy(fresh_v.at[b], fresh_out.at[b], sem.at[2 * i + 1]))
    for copy in copies:
        copy.start()
    for copy in copies:
        copy.wait()


def level_size(n_mp):
    size = 1
    while size * size < n_mp:
        size *= 2
    return size


def local(n_dp, n_mp, grad_parts, factors, root_prev, plan):
    blocks, bs = grad_parts.shape[2], factors.shape[-1]
    high = bs // n_mp
    row = level_size(n_mp)
    wide = bs // GROUPS
    grads = grad_parts.reshape(blocks, bs, bs)
    old = root_prev.reshape(n_mp, high, bs)
    fresh, new_factor = pl.pallas_call(
        functools.partial(kernel, n_dp, n_mp, blocks, row),
        out_shape=(
            pltpu.VMEM((n_mp, high, bs), BF16),
            pltpu.VMEM((bs, bs), F32),
        ),
        in_specs=[pl.BlockSpec(memory_space=pl.ANY)] * 4,
        out_specs=(pl.BlockSpec(memory_space=pltpu.VMEM),) * 2,
        scratch_shapes=[
            pltpu.SMEM(plan.shape, plan.dtype),
            pltpu.VMEM((bs, bs), BF16),
            pltpu.VMEM((n_dp - 1, bs, bs), BF16),
            pltpu.VMEM((bs, bs), F32),
            pltpu.VMEM((n_mp, high, bs), BF16),
            pltpu.VMEM((bs, bs), BF16),
            pltpu.VMEM((bs, bs), F32),
            pltpu.VMEM((bs, bs), BF16),
            pltpu.VMEM((bs, bs), BF16),
            pltpu.VMEM((bs, bs), BF16),
            pltpu.VMEM((bs, bs), BF16),
            pltpu.VMEM((n_mp, high, bs), BF16),
            pltpu.SemaphoreType.DMA((4,)),
            pltpu.SemaphoreType.DMA((2,)),
            pltpu.SemaphoreType.DMA((GROUPS,)),
            pltpu.SemaphoreType.DMA((GROUPS,)),
            pltpu.SemaphoreType.DMA((GROUPS,)),
            pltpu.SemaphoreType.DMA,
            pltpu.SemaphoreType.DMA,
            pltpu.SemaphoreType.DMA,
            pltpu.SemaphoreType.DMA,
            pltpu.SemaphoreType.REGULAR((n_mp // row,)),
        ],
        compiler_params=pltpu.CompilerParams(collective_id=0, has_side_effects=True),
        name="refresh",
    )(plan, grads, factors.reshape(bs, bs), old)
    new_factor, fresh = pl.pallas_call(
        write_out,
        out_shape=(
            jax.ShapeDtypeStruct((bs, bs), F32),
            jax.ShapeDtypeStruct((n_mp, high, bs), BF16),
        ),
        in_specs=[pl.BlockSpec(memory_space=pl.ANY)] * 2,
        out_specs=(pl.BlockSpec(memory_space=pl.ANY),) * 2,
        scratch_shapes=[pltpu.SemaphoreType.DMA((8,))],
        compiler_params=pltpu.CompilerParams(vmem_limit_bytes=1 << 20),
        name="write_out",
    )(new_factor, fresh)
    return (new_factor[None, None], fresh.reshape(root_prev.shape))


def solution(mesh):
    return jax.shard_map(
        functools.partial(local, mesh.shape["dp"], mesh.shape["mp"]),
        mesh=mesh,
        in_specs=(
            P("dp", "mp", None, None, None),
            P("mp", "dp", None, None),
            P(None, "dp", "mp", None),
            P("dp", None),
        ),
        out_specs=(P("mp", "dp", None, None), P(None, "dp", "mp", None)),
        check_vma=False,
    )
```

```python
import functools

import jax
import jax.numpy as jnp
from jax import lax
from jax.experimental import pallas as pl
from jax.experimental.pallas import tpu as pltpu
from jax.sharding import PartitionSpec as P

keep_rate = 0.8
fresh_rate = 1.0 - keep_rate
GROUPS = 4
MESH = pl.DeviceIdType.MESH
F32 = jnp.float32
BF16 = jnp.bfloat16
scope = jax.named_scope


def mul(a, b, dims=(1, 0)):
    return lax.dot_general(a, b, (((dims[0],), (dims[1],)), ((), ())), preferred_element_type=F32)


def wait_bytes(ref, sem):
    pltpu.make_async_copy(ref, ref, sem).wait()


def kernel(
    n_dp, n_mp, blocks, row,
    plan, grad, fac, root, fresh, fac_out, plan_s,
    own_g, in_g, fac_v, pieces, full_x, rest, fifth, fac_b, summed, gram_b, out_v,
    load_sem, grad_send, grad_recv, gram_send, gram_recv, root_send, root_recv, out_send, out_recv, above,
):
    d = lax.axis_index("dp")
    me = lax.axis_index("mp")
    bs = fac.shape[-1]
    high = bs // n_mp
    half = n_mp // 2
    hb = bs // 2
    wide = bs // GROUPS
    levels = n_mp // row
    level = me // row
    at = me % row
    band = row // 2
    upper_band = at >= band
    start = me - at % band
    side = me // half
    away = 1 - side
    near_cols = pl.ds(pl.multiple_of(side * hb, hb), hb)
    far_cols = pl.ds(pl.multiple_of(away * hb, hb), hb)
    far_first = pl.ds(pl.multiple_of(away * hb, hb), hb // 2)
    far_second = pl.ds(pl.multiple_of(away * hb + hb // 2, hb // 2), hb // 2)
    near_pieces = pl.ds(side * half, half)
    far_pieces = pl.ds(away * half, half)
    parity = me % 2
    collects = d % 2 == parity
    partner = d + 1 - 2 * (d % 2)

    loads = [
        pltpu.make_async_copy(grad.at[d // 2], own_g, load_sem.at[0]),
        pltpu.make_async_copy(root.at[me], pieces.at[me], load_sem.at[1]),
        pltpu.make_async_copy(fac, fac_v, load_sem.at[2]),
        pltpu.make_async_copy(plan, plan_s, load_sem.at[3]),
    ]

    def signal(sem, dp, mp):
        pl.semaphore_signal(sem, inc=1, device_id=(dp, mp), device_id_type=MESH)

    def by_parity(act):
        @pl.when(parity == 0)
        def _():
            act(True)

        @pl.when(parity == 1)
        def _():
            act(False)

    with scope("BARRIER"):
        barrier = pltpu.get_barrier_semaphore()
        for i in range(1, n_dp):
            signal(barrier, (d + i) % n_dp, me)
        for i in range(1, band):
            signal(barrier, d, start + (at + i) % band)
        for k in range(1, levels):
            @pl.when(level + k < levels)
            def _():
                for i in range(band):
                    signal(barrier, d, start + k * row + (at + i) % band)

        @pl.when(jnp.logical_not(upper_band))
        def _():
            for k in range(levels):
                @pl.when(level + k < levels)
                def _():
                    for i in range(band):
                        signal(barrier, d, start + k * row + band + (at + i) % band)

        for load in loads:
            load.start()
        known = n_dp - 1 + band - 1 + level * band
        pl.semaphore_wait(barrier, jnp.where(upper_band, known + (level + 1) * band, known))

        @pl.when(upper_band)
        def _():
            for k in range(levels):
                @pl.when(level >= k)
                def _():
                    signal(above.at[k], d, me - k * row - band)
                    if k:
                        signal(above.at[k], d, me - k * row)

    def strip(ref, c, by_cols):
        cut = pl.ds(c * wide, wide)
        return ref.at[:, cut] if by_cols else ref.at[cut, :]

    def send_grads(by_cols):
        for c in range(GROUPS):
            for k in range(blocks):
                to = 2 * k + parity

                @pl.when(to != d)
                def _():
                    pltpu.make_async_remote_copy(
                        src_ref=strip(grad.at[k], c, by_cols),
                        dst_ref=strip(in_g.at[(d - to + n_dp) % n_dp - 1], c, by_cols),
                        send_sem=grad_send.at[c // (GROUPS - 1)], recv_sem=grad_recv.at[c],
                        device_id=(to, me), device_id_type=MESH,
                    ).start()

    by_parity(send_grads)

    def root_far(t):
        base = side * hb
        upper = me % half < half // 2

        def copy(start, size):
            cols = pl.ds(pl.multiple_of(start, hb // 2), size)
            pltpu.make_async_remote_copy(
                src_ref=root.at[t, :, cols], dst_ref=pieces.at[me, :, cols],
                send_sem=root_send, recv_sem=root_recv, device_id=(d, t), device_id_type=MESH,
            ).start()

        @pl.when(upper)
        def _():
            copy(base, hb)

        @pl.when(jnp.logical_not(upper))
        def _():
            copy(base + hb // 2, hb // 2)

    def root_near(t):
        pltpu.make_async_remote_copy(
            src_ref=root.at[t], dst_ref=pieces.at[me],
            send_sem=root_send, recv_sem=root_recv, device_id=(d, t), device_id_type=MESH,
        ).start()

    def send_roots(to, odd):
        for j in range(band // 2):
            t = to + (at // 2 * 2 + 2 * j) % band + odd
            close = t // half == side

            @pl.when(jnp.logical_not(close))
            def _():
                root_far(t)

            @pl.when(jnp.logical_and(close, t != me))
            def _():
                root_near(t)

    def each_level(odd, meet):
        for k in reversed(range(levels)):
            @pl.when(level >= k)
            def _():
                send_roots((level - k) * row, odd)

        if meet:
            @pl.when(jnp.logical_not(upper_band))
            def _():
                pl.semaphore_wait(above.at[0], 1)

        for k in reversed(range(levels)):
            @pl.when(level >= k)
            def _():
                send_roots((level - k) * row + band, odd)

        for k in range(1, levels):
            @pl.when(level + k < levels)
            def _():
                if meet:
                    pl.semaphore_wait(above.at[k], 1)
                send_roots((level + k) * row, odd)
                send_roots((level + k) * row + band, odd)

    with scope("ROOTSEND"):
        each_level(d % 2, True)

    def take(c, by_cols):
        wait_bytes(in_g.at[:, :, pl.ds(c * wide, wide)] if by_cols else in_g.at[:, pl.ds(c * wide, wide), :], grad_recv.at[c])
        total = strip(own_g, c, by_cols)[...].astype(F32)
        for i in range(n_dp - 1):
            total += strip(in_g.at[i], c, by_cols)[...].astype(F32)
        strip(summed, c, by_cols)[...] = total.astype(BF16)

    def make_row(c, by_cols):
        new = strip(summed, c, by_cols)[...]
        so_far = pl.ds(0, (c + 1) * wide)
        product = mul(new, summed[:, so_far], (0, 0)) if by_cols else mul(new, summed[so_far, :], (1, 1))
        gram_b[pl.ds(c * wide, wide), so_far] = (fresh_rate * product).astype(BF16)

    def gram_row(c):
        part = gram_b.at[pl.ds(c * wide, wide), pl.ds(0, (c + 1) * wide)]
        return pltpu.make_async_remote_copy(
            src_ref=part, dst_ref=part, send_sem=gram_send.at[c], recv_sem=gram_recv.at[c],
            device_id=(partner, me), device_id_type=MESH,
        )

    early = GROUPS // 2
    loads[0].wait()

    with scope("EARLY"):
        @pl.when(collects)
        def _():
            def act(by_cols):
                for c in range(early):
                    take(c, by_cols)
                    make_row(c, by_cols)
                    if c == 0:
                        each_level(1 - d % 2, False)

            by_parity(act)

        @pl.when(jnp.logical_not(collects))
        def _():
            wait_bytes(in_g.at[pl.ds(0, blocks), pl.ds(0, bs - wide), :], grad_send.at[0])
            each_level(1 - d % 2, False)

    with scope("ROOTRECV"):
        loads[1].wait()
        loads[2].wait()
        wait_bytes(pieces.at[pl.ds(0, half - 1 + half * 3 // 8)], root_recv)

    loads[3].wait()
    kept = plan_s[0, me] >= n_mp
    x_rate = jnp.where(kept, 1.0, 1.25)
    step = jnp.where(kept, 0.0, 0.25)

    with scope("ASSEMBLE"):
        near_rows = pieces[near_pieces].astype(F32).reshape(hb, bs).astype(BF16)
        full_x[near_cols, :] = near_rows
        full_x[far_cols, far_cols] = pieces[far_pieces, :, far_cols].astype(F32).reshape(hb, hb).astype(BF16)
        full_x[far_second, far_first] = full_x[far_first, far_second].astype(F32).T.astype(BF16)
        full_x[far_cols, near_cols] = full_x[near_cols, far_cols].astype(F32).T.astype(BF16)

    with scope("CHAIN"):
        x = full_x[...]
        square = mul(x, x).astype(BF16)
        fourth = mul(square, square).astype(BF16)
        fifth[...] = (step * mul(x, fourth)).astype(BF16)

    def send_out(t):
        pltpu.make_async_remote_copy(
            src_ref=out_v.at[t], dst_ref=fresh.at[me],
            send_sem=out_send, recv_sem=out_recv, device_id=(d, t), device_id_type=MESH,
        ).start()

    def refine(first, count, base, factor):
        rows = pl.ds(pl.multiple_of(first * high, high), count * high)
        refined = base(rows) - mul(fifth[rows, :], factor[...])
        out_v[pl.ds(first, count)] = refined.reshape(count, high, bs).astype(BF16)

    def give_far(base, factor):
        for k in range(half // row):
            refine(away * half + k * row, row, base, factor)
            for j in range(row):
                send_out(away * half + k * row + j // 2 * 2 + (j + at) % 2)

    def give_near(base, factor):
        refine(side * half, half, base, factor)

        @pl.loop(1, half)
        def _(i):
            send_out(side * half + (me + i) % half)

    def part_x(rows):
        return x_rate * full_x[rows, :].astype(F32)

    @pl.when(collects)
    def _():
        def act(by_cols):
            dims = (1, 1) if by_cols else (0, 0)
            last = GROUPS - 1
            with scope("GRADS"):
                for c in range(early, last):
                    take(c, by_cols)
                for c in range(early):
                    gram_row(c).start()
                cut = pl.ds(0, last * wide)
                known = summed[:, cut] if by_cols else summed[cut, :]
                fac_out[...] = keep_rate * fac_v[...] + fresh_rate * mul(known, known, dims)
            with scope("GRADLAST"):
                take(last, by_cols)
                new = strip(summed, last, by_cols)[...]
                fac_b[...] = (fac_out[...] + fresh_rate * mul(new, new, dims)).astype(BF16)
            with scope("GIVEFAR"):
                give_far(part_x, fac_b)
            with scope("ROWLAST"):
                for c in range(early, GROUPS):
                    make_row(c, by_cols)
                    gram_row(c).start()
            with scope("GIVENEAR"):
                give_near(part_x, fac_b)
            with scope("FACOUT"):
                fac_out[...] += fresh_rate * mul(new, new, dims)
            for c in range(GROUPS):
                gram_row(c).wait_send()

        by_parity(act)

    @pl.when(jnp.logical_not(collects))
    def _():
        with scope("REST"):
            rest[...] = x_rate * full_x[...].astype(F32) - keep_rate * mul(fifth[...], fac_v[...].astype(BF16))
        for c in range(GROUPS):
            with scope("GRAMIN%d" % c):
                gram_row(c).wait_recv()
                if c:
                    rows = pl.ds(c * wide, wide)
                    before = pl.ds(0, c * wide)
                    gram_b[before, rows] = gram_b[rows, before].astype(F32).T.astype(BF16)
        with scope("GIVEFAR"):
            give_far(lambda rows: rest[rows, :], gram_b)
        with scope("GIVENEAR"):
            give_near(lambda rows: rest[rows, :], gram_b)
        with scope("FACOUT"):
            fac_out[...] = keep_rate * fac_v[...] + gram_b[...].astype(F32)
            wait_bytes(in_g.at[pl.ds(0, blocks), pl.ds(0, wide), :], grad_send.at[1])

    with scope("SENDS"):
        own_out = pltpu.make_async_copy(out_v.at[me], fresh.at[me], load_sem.at[0])
        own_out.start()
        if blocks > 1:
            @pl.when(collects)
            def _():
                wait_bytes(in_g.at[pl.ds(0, blocks - 1), pl.ds(0, bs - wide), :], grad_send.at[0])
                wait_bytes(in_g.at[pl.ds(0, blocks - 1), pl.ds(0, wide), :], grad_send.at[1])

        @pl.when(me % half < half // 2)
        def _():
            wait_bytes(pieces.at[pl.ds(0, half - 1 + half // 2)], root_send)

        @pl.when(me % half >= half // 2)
        def _():
            wait_bytes(pieces.at[pl.ds(0, half - 1 + half // 4)], root_send)

        own_out.wait()
        wait_bytes(out_v.at[pl.ds(0, n_mp - 1)], out_send)

    with scope("RECV"):
        wait_bytes(fresh.at[pl.ds(0, n_mp - 1)], out_recv)


def write_out(fac_v, fresh_v, fac_out, fresh_out, sem):
    n = 4
    copies = []
    for i in range(n):
        a = pl.ds(i * (fac_v.shape[0] // n), fac_v.shape[0] // n)
        b = pl.ds(i * (fresh_v.shape[0] // n), fresh_v.shape[0] // n)
        copies.append(pltpu.make_async_copy(fac_v.at[a], fac_out.at[a], sem.at[2 * i]))
        copies.append(pltpu.make_async_copy(fresh_v.at[b], fresh_out.at[b], sem.at[2 * i + 1]))
    for copy in copies:
        copy.start()
    for copy in copies:
        copy.wait()


def level_size(n_mp):
    size = 1
    while size * size < n_mp:
        size *= 2
    return size


def local(n_dp, n_mp, grad_parts, factors, root_prev, plan):
    blocks, bs = grad_parts.shape[2], factors.shape[-1]
    high = bs // n_mp
    row = level_size(n_mp)
    wide = bs // GROUPS
    grads = grad_parts.reshape(blocks, bs, bs)
    old = root_prev.reshape(n_mp, high, bs)
    fresh, new_factor = pl.pallas_call(
        functools.partial(kernel, n_dp, n_mp, blocks, row),
        out_shape=(
            pltpu.VMEM((n_mp, high, bs), BF16),
            pltpu.VMEM((bs, bs), F32),
        ),
        in_specs=[pl.BlockSpec(memory_space=pl.ANY)] * 4,
        out_specs=(pl.BlockSpec(memory_space=pltpu.VMEM),) * 2,
        scratch_shapes=[
            pltpu.SMEM(plan.shape, plan.dtype),
            pltpu.VMEM((bs, bs), BF16),
            pltpu.VMEM((n_dp - 1, bs, bs), BF16),
            pltpu.VMEM((bs, bs), F32),
            pltpu.VMEM((n_mp, high, bs), BF16),
            pltpu.VMEM((bs, bs), BF16),
            pltpu.VMEM((bs, bs), F32),
            pltpu.VMEM((bs, bs), BF16),
            pltpu.VMEM((bs, bs), BF16),
            pltpu.VMEM((bs, bs), BF16),
            pltpu.VMEM((bs, bs), BF16),
            pltpu.VMEM((n_mp, high, bs), BF16),
            pltpu.SemaphoreType.DMA((4,)),
            pltpu.SemaphoreType.DMA((2,)),
            pltpu.SemaphoreType.DMA((GROUPS,)),
            pltpu.SemaphoreType.DMA((GROUPS,)),
            pltpu.SemaphoreType.DMA((GROUPS,)),
            pltpu.SemaphoreType.DMA,
            pltpu.SemaphoreType.DMA,
            pltpu.SemaphoreType.DMA,
            pltpu.SemaphoreType.DMA,
            pltpu.SemaphoreType.REGULAR((n_mp // row,)),
        ],
        compiler_params=pltpu.CompilerParams(collective_id=0, has_side_effects=True),
        name="refresh",
    )(plan, grads, factors.reshape(bs, bs), old)
    new_factor, fresh = pl.pallas_call(
        write_out,
        out_shape=(
            jax.ShapeDtypeStruct((bs, bs), F32),
            jax.ShapeDtypeStruct((n_mp, high, bs), BF16),
        ),
        in_specs=[pl.BlockSpec(memory_space=pl.ANY)] * 2,
        out_specs=(pl.BlockSpec(memory_space=pl.ANY),) * 2,
        scratch_shapes=[pltpu.SemaphoreType.DMA((8,))],
        compiler_params=pltpu.CompilerParams(vmem_limit_bytes=1 << 20),
        name="write_out",
    )(new_factor, fresh)
    return (new_factor[None, None], fresh.reshape(root_prev.shape))


def solution(mesh):
    return jax.shard_map(
        functools.partial(local, mesh.shape["dp"], mesh.shape["mp"]),
        mesh=mesh,
        in_specs=(
            P("dp", "mp", None, None, None),
            P("mp", "dp", None, None),
            P(None, "dp", "mp", None),
            P("dp", None),
        ),
        out_specs=(P("mp", "dp", None, None), P(None, "dp", "mp", None)),
        check_vma=False,
    )
```

```python
import functools

import jax
import jax.numpy as jnp
from jax import lax
from jax.experimental import pallas as pl
from jax.experimental.pallas import tpu as pltpu
from jax.sharding import PartitionSpec as P

keep_rate = 0.8
fresh_rate = 1.0 - keep_rate
GROUPS = 4
MESH = pl.DeviceIdType.MESH
F32 = jnp.float32
BF16 = jnp.bfloat16
scope = jax.named_scope


def mul(a, b, dims=(1, 0)):
    return lax.dot_general(a, b, (((dims[0],), (dims[1],)), ((), ())), preferred_element_type=F32)


def wait_bytes(ref, sem):
    pltpu.make_async_copy(ref, ref, sem).wait()


def kernel(
    n_dp, n_mp, blocks, row,
    plan, grad, fac, root, fresh, fac_out, plan_s,
    own_g, in_g, fac_v, pieces, full_x, rest, fifth, fac_b, summed, gram_b, out_v,
    load_sem, grad_send, grad_recv, gram_send, gram_recv, root_send, root_recv, out_send, out_recv, ready, above,
):
    d = lax.axis_index("dp")
    me = lax.axis_index("mp")
    bs = fac.shape[-1]
    high = bs // n_mp
    half = n_mp // 2
    hb = bs // 2
    wide = bs // GROUPS
    levels = n_mp // row
    level = me // row
    at = me % row
    band = row // 2
    upper_band = at >= band
    start = me - at % band
    side = me // half
    away = 1 - side
    near_cols = pl.ds(pl.multiple_of(side * hb, hb), hb)
    far_cols = pl.ds(pl.multiple_of(away * hb, hb), hb)
    far_first = pl.ds(pl.multiple_of(away * hb, hb), hb // 2)
    far_second = pl.ds(pl.multiple_of(away * hb + hb // 2, hb // 2), hb // 2)
    near_pieces = pl.ds(side * half, half)
    far_pieces = pl.ds(away * half, half)
    parity = me % 2
    collects = d % 2 == parity
    partner = d + 1 - 2 * (d % 2)

    loads = [
        pltpu.make_async_copy(root.at[me], pieces.at[me], load_sem.at[0]),
        pltpu.make_async_copy(fac, fac_v, load_sem.at[1]),
        pltpu.make_async_copy(plan, plan_s, load_sem.at[2]),
        pltpu.make_async_copy(grad.at[d // 2], own_g, load_sem.at[3]),
    ]

    def signal(sem, dp, mp):
        pl.semaphore_signal(sem, inc=1, device_id=(dp, mp), device_id_type=MESH)

    def strip(ref, c, by_cols):
        cut = pl.ds(c * wide, wide)
        return ref.at[:, cut] if by_cols else ref.at[cut, :]

    def strips(ref, c, by_cols):
        cut = pl.ds(c * wide, wide)
        return ref.at[:, :, cut] if by_cols else ref.at[:, cut, :]

    def by_parity(act):
        @pl.when(parity == 0)
        def _():
            act(True)

        @pl.when(parity == 1)
        def _():
            act(False)

    def send_grads(by_cols):
        for c in range(GROUPS):
            for k in range(blocks):
                to = 2 * k + parity

                @pl.when(to != d)
                def _():
                    pltpu.make_async_remote_copy(
                        src_ref=strip(grad.at[k], c, by_cols),
                        dst_ref=strip(in_g.at[(d - to + n_dp) % n_dp - 1], c, by_cols),
                        send_sem=grad_send.at[c // (GROUPS - 1)], recv_sem=grad_recv.at[c],
                        device_id=(to, me), device_id_type=MESH,
                    ).start()

    with scope("BARRIER"):
        barrier = pltpu.get_barrier_semaphore()
        odd_sender = jnp.logical_and(jnp.logical_not(collects), d % 2 == 1)

        @pl.when(collects)
        def _():
            for i in range(1, n_dp):
                signal(barrier, (d + i) % n_dp, me)

        @pl.when(odd_sender)
        def _():
            pl.semaphore_wait(barrier, blocks)
            send_grads(True)

        def greet(first):
            for i in range(band // 2):
                t = first + 2 * i + d % 2

                @pl.when(t != me)
                def _():
                    signal(barrier, d, t)

        for k in range(levels):
            @pl.when(level + k < levels)
            def _():
                greet(start + k * row)

                @pl.when(jnp.logical_not(upper_band))
                def _():
                    greet(start + k * row + band)

        @pl.when(collects)
        def _():
            loads[3].start()

        known = blocks - 1 + band - 1 + level * band + jnp.where(upper_band, (level + 1) * band, 0)

        @pl.when(jnp.logical_and(jnp.logical_not(collects), d % 2 == 0))
        def _():
            pl.semaphore_wait(barrier, blocks)
            send_grads(False)

        @pl.when(collects)
        def _():
            pl.semaphore_wait(barrier, known)
            if blocks > 1:
                by_parity(send_grads)
            signal(ready, d, me + 1 - 2 * parity)

        @pl.when(jnp.logical_and(upper_band, collects))
        def _():
            for k in range(levels):
                @pl.when(level >= k)
                def _():
                    pair = me - at % 2 - k * row
                    for i in range(2):
                        signal(above.at[k], d, pair - band + i)
                        if k:
                            signal(above.at[k], d, pair + i)

    def root_far(t):
        base = side * hb
        upper = me % half < half // 2

        def copy(start, size):
            cols = pl.ds(pl.multiple_of(start, hb // 2), size)
            pltpu.make_async_remote_copy(
                src_ref=root.at[t, :, cols], dst_ref=pieces.at[me, :, cols],
                send_sem=root_send, recv_sem=root_recv, device_id=(d, t), device_id_type=MESH,
            ).start()

        @pl.when(upper)
        def _():
            copy(base, hb)

        @pl.when(jnp.logical_not(upper))
        def _():
            copy(base + hb // 2, hb // 2)

    def root_near(t):
        pltpu.make_async_remote_copy(
            src_ref=root.at[t], dst_ref=pieces.at[me],
            send_sem=root_send, recv_sem=root_recv, device_id=(d, t), device_id_type=MESH,
        ).start()

    def send_roots(to, odd):
        for j in range(band // 2):
            t = to + (at // 2 * 2 + 2 * j) % band + odd
            close = t // half == side

            @pl.when(jnp.logical_not(close))
            def _():
                root_far(t)

            @pl.when(jnp.logical_and(close, t != me))
            def _():
                root_near(t)

    def each_level(odd, meet):
        for k in reversed(range(levels)):
            @pl.when(level >= k)
            def _():
                send_roots((level - k) * row, odd)

        if meet:
            @pl.when(jnp.logical_not(upper_band))
            def _():
                pl.semaphore_wait(above.at[0], 1)

        for k in reversed(range(levels)):
            @pl.when(level >= k)
            def _():
                send_roots((level - k) * row + band, odd)

        for k in range(1, levels):
            @pl.when(level + k < levels)
            def _():
                if meet:
                    pl.semaphore_wait(above.at[k], 1)
                send_roots((level + k) * row, odd)
                send_roots((level + k) * row + band, odd)

    with scope("ROOTSEND"):
        @pl.when(jnp.logical_not(collects))
        def _():
            pl.semaphore_wait(ready, 1)

        each_level(d % 2, True)
        for load in loads[:3]:
            load.start()

    def take(c, by_cols):
        wait_bytes(strips(in_g, c, by_cols), grad_recv.at[c])
        total = strip(own_g, c, by_cols)[...].astype(F32)
        for i in range(n_dp - 1):
            total += strip(in_g.at[i], c, by_cols)[...].astype(F32)
        strip(summed, c, by_cols)[...] = total.astype(BF16)

    def make_row(c, by_cols):
        new = strip(summed, c, by_cols)[...]
        so_far = pl.ds(0, (c + 1) * wide)
        product = mul(new, summed[:, so_far], (0, 0)) if by_cols else mul(new, summed[so_far, :], (1, 1))
        gram_b[pl.ds(c * wide, wide), so_far] = (fresh_rate * product).astype(BF16)

    def gram_row(c):
        part = gram_b.at[pl.ds(c * wide, wide), pl.ds(0, (c + 1) * wide)]
        return pltpu.make_async_remote_copy(
            src_ref=part, dst_ref=part, send_sem=gram_send, recv_sem=gram_recv.at[c // (GROUPS - 1)],
            device_id=(partner, me), device_id_type=MESH,
        )

    early = GROUPS // 2
    with scope("EARLY"):
        @pl.when(collects)
        def _():
            loads[3].wait()

            def act(by_cols):
                for c in range(early):
                    take(c, by_cols)
                    make_row(c, by_cols)
                    if c == 0:
                        each_level(1 - d % 2, False)

            by_parity(act)

        @pl.when(jnp.logical_not(collects))
        def _():
            wait_bytes(in_g.at[pl.ds(0, blocks), pl.ds(0, bs - wide), :], grad_send.at[0])
            each_level(1 - d % 2, False)

    with scope("ROOTRECV"):
        loads[0].wait()
        loads[1].wait()
        wait_bytes(pieces.at[pl.ds(0, half - 1 + half * 3 // 8)], root_recv)

    loads[2].wait()
    kept = plan_s[0, me] >= n_mp
    x_rate = jnp.where(kept, 1.0, 1.25)
    step = jnp.where(kept, 0.0, 0.25)

    with scope("ASSEMBLE"):
        near_rows = pieces[near_pieces].astype(F32).reshape(hb, bs).astype(BF16)
        full_x[near_cols, :] = near_rows
        full_x[far_cols, far_cols] = pieces[far_pieces, :, far_cols].astype(F32).reshape(hb, hb).astype(BF16)
        full_x[far_second, far_first] = full_x[far_first, far_second].astype(F32).T.astype(BF16)
        full_x[far_cols, near_cols] = full_x[near_cols, far_cols].astype(F32).T.astype(BF16)

    with scope("CHAIN"):
        x = full_x[...]
        square = mul(x, x).astype(BF16)
        fourth = mul(square, square).astype(BF16)
        fifth[...] = (step * mul(x, fourth)).astype(BF16)

    def send_out(t):
        pltpu.make_async_remote_copy(
            src_ref=out_v.at[t], dst_ref=fresh.at[me],
            send_sem=out_send, recv_sem=out_recv, device_id=(d, t), device_id_type=MESH,
        ).start()

    def refine(first, count, value):
        rows = pl.ds(pl.multiple_of(first * high, high), count * high)
        out_v[pl.ds(first, count)] = value(rows).reshape(count, high, bs).astype(BF16)

    def give_far(k, value):
        to = away * half + k * row
        refine(to, row, value)
        for j in range(row):
            turn = jnp.where(to == 0, j // band, (j // band + 1 + upper_band.astype(jnp.int32)) % 2)
            send_out(to + turn * band + (at + j) % band)

    def give_near(value):
        refine(side * half, half, value)

        @pl.loop(1, half)
        def _(i):
            send_out(side * half + (me + i) % half)

    def with_factor(rows):
        return x_rate * full_x[rows, :].astype(F32) - mul(fifth[rows, :], fac_b[...])

    @pl.when(collects)
    def _():
        def act(by_cols):
            dims = (1, 1) if by_cols else (0, 0)
            across = (1, 0) if by_cols else (1, 1)
            back = (1, 1) if by_cols else (1, 0)
            last = GROUPS - 1
            first_rows = pl.ds(pl.multiple_of(away * hb, hb), row * high)
            with scope("GRADS"):
                for c in range(early, last):
                    take(c, by_cols)
                    make_row(c, by_cols)
                for c in range(last):
                    gram_row(c).start()
                cut = pl.ds(0, last * wide)
                known = summed[:, cut] if by_cols else summed[cut, :]
                total = keep_rate * fac_v[...] + fresh_rate * mul(known, known, dims)
                fac_out[...] = total
                fac_b[...] = total.astype(BF16)
                rest[first_rows, :] = with_factor(first_rows)
            with scope("GRADLAST"):
                take(last, by_cols)
                new = strip(summed, last, by_cols)[...]
                turned = (fresh_rate * mul(fifth[first_rows, :], new, across)).astype(BF16)
                give_far(0, lambda rows: rest[rows, :] - mul(turned, new, back))
            with scope("ROWLAST"):
                make_row(last, by_cols)
                gram_row(last).start()
            with scope("GIVEFAR"):
                fac_b[...] = (fac_out[...] + fresh_rate * mul(new, new, dims)).astype(BF16)
                for k in range(1, half // row):
                    give_far(k, with_factor)
            with scope("GIVENEAR"):
                give_near(with_factor)
            with scope("FACOUT"):
                fac_out[...] += fresh_rate * mul(new, new, dims)
            wait_bytes(gram_b.at[pl.ds(0, bs * (GROUPS + 1) // (2 * GROUPS))], gram_send)

        by_parity(act)

    @pl.when(jnp.logical_not(collects))
    def _():
        with scope("REST"):
            rest[...] = x_rate * full_x[...].astype(F32) - keep_rate * mul(fifth[...], fac_v[...].astype(BF16))
        def mirror(c):
            rows = pl.ds(c * wide, wide)
            before = pl.ds(0, c * wide)
            gram_b[before, rows] = gram_b[rows, before].astype(F32).T.astype(BF16)

        last = GROUPS - 1
        with scope("GRAMIN"):
            wait_bytes(gram_b.at[pl.ds(0, last * wide), pl.ds(0, bs // 2)], gram_recv.at[0])
            for c in range(1, last):
                mirror(c)
        with scope("GRAMLAST"):
            gram_row(last).wait_recv()
            mirror(last)

        def with_gram(rows):
            return rest[rows, :] - mul(fifth[rows, :], gram_b[...])

        with scope("GIVEFAR"):
            for k in range(half // row):
                give_far(k, with_gram)
        with scope("GIVENEAR"):
            give_near(with_gram)
        with scope("FACOUT"):
            fac_out[...] = keep_rate * fac_v[...] + gram_b[...].astype(F32)
            wait_bytes(in_g.at[pl.ds(0, blocks), pl.ds(0, wide), :], grad_send.at[1])

    with scope("SENDS"):
        own_out = pltpu.make_async_copy(out_v.at[me], fresh.at[me], load_sem.at[0])
        own_out.start()
        if blocks > 1:
            @pl.when(collects)
            def _():
                wait_bytes(in_g.at[pl.ds(0, blocks - 1), pl.ds(0, bs - wide), :], grad_send.at[0])
                wait_bytes(in_g.at[pl.ds(0, blocks - 1), pl.ds(0, wide), :], grad_send.at[1])

        @pl.when(me % half < half // 2)
        def _():
            wait_bytes(pieces.at[pl.ds(0, half - 1 + half // 2)], root_send)

        @pl.when(me % half >= half // 2)
        def _():
            wait_bytes(pieces.at[pl.ds(0, half - 1 + half // 4)], root_send)

        own_out.wait()
        wait_bytes(out_v.at[pl.ds(0, n_mp - 1)], out_send)

    with scope("RECV"):
        wait_bytes(fresh.at[pl.ds(0, n_mp - 1)], out_recv)


def write_out(fac_v, fresh_v, fac_out, fresh_out, sem):
    copies = [
        pltpu.make_async_copy(fac_v, fac_out, sem.at[0]),
        pltpu.make_async_copy(fresh_v, fresh_out, sem.at[1]),
    ]
    for copy in copies:
        copy.start()
    for copy in copies:
        copy.wait()


def level_size(n_mp):
    size = 1
    while size * size < n_mp:
        size *= 2
    return size


def local(n_dp, n_mp, grad_parts, factors, root_prev, plan):
    blocks, bs = grad_parts.shape[2], factors.shape[-1]
    high = bs // n_mp
    row = level_size(n_mp)
    wide = bs // GROUPS
    grads = grad_parts.reshape(blocks, bs, bs)
    old = root_prev.reshape(n_mp, high, bs)
    fresh, new_factor = pl.pallas_call(
        functools.partial(kernel, n_dp, n_mp, blocks, row),
        out_shape=(
            pltpu.VMEM((n_mp, high, bs), BF16),
            pltpu.VMEM((bs, bs), F32),
        ),
        in_specs=[pl.BlockSpec(memory_space=pl.ANY)] * 4,
        out_specs=(pl.BlockSpec(memory_space=pltpu.VMEM),) * 2,
        scratch_shapes=[
            pltpu.SMEM(plan.shape, plan.dtype),
            pltpu.VMEM((bs, bs), BF16),
            pltpu.VMEM((n_dp - 1, bs, bs), BF16),
            pltpu.VMEM((bs, bs), F32),
            pltpu.VMEM((n_mp, high, bs), BF16),
            pltpu.VMEM((bs, bs), BF16),
            pltpu.VMEM((bs, bs), F32),
            pltpu.VMEM((bs, bs), BF16),
            pltpu.VMEM((bs, bs), BF16),
            pltpu.VMEM((bs, bs), BF16),
            pltpu.VMEM((bs, bs), BF16),
            pltpu.VMEM((n_mp, high, bs), BF16),
            pltpu.SemaphoreType.DMA((4,)),
            pltpu.SemaphoreType.DMA((2,)),
            pltpu.SemaphoreType.DMA((GROUPS,)),
            pltpu.SemaphoreType.DMA,
            pltpu.SemaphoreType.DMA((2,)),
            pltpu.SemaphoreType.DMA,
            pltpu.SemaphoreType.DMA,
            pltpu.SemaphoreType.DMA,
            pltpu.SemaphoreType.DMA,
            pltpu.SemaphoreType.REGULAR,
            pltpu.SemaphoreType.REGULAR((n_mp // row,)),
        ],
        compiler_params=pltpu.CompilerParams(collective_id=0, has_side_effects=True),
        name="refresh",
    )(plan, grads, factors.reshape(bs, bs), old)
    new_factor, fresh = pl.pallas_call(
        write_out,
        out_shape=(
            jax.ShapeDtypeStruct((bs, bs), F32),
            jax.ShapeDtypeStruct((n_mp, high, bs), BF16),
        ),
        in_specs=[pl.BlockSpec(memory_space=pl.ANY)] * 2,
        out_specs=(pl.BlockSpec(memory_space=pl.ANY),) * 2,
        scratch_shapes=[pltpu.SemaphoreType.DMA((2,))],
        compiler_params=pltpu.CompilerParams(vmem_limit_bytes=1 << 20),
        name="write_out",
    )(new_factor, fresh)
    return (new_factor[None, None], fresh.reshape(root_prev.shape))


def solution(mesh):
    return jax.shard_map(
        functools.partial(local, mesh.shape["dp"], mesh.shape["mp"]),
        mesh=mesh,
        in_specs=(
            P("dp", "mp", None, None, None),
            P("mp", "dp", None, None),
            P(None, "dp", "mp", None),
            P("dp", None),
        ),
        out_specs=(P("mp", "dp", None, None), P(None, "dp", "mp", None)),
        check_vma=False,
    )
```

```python
import functools

import jax
import jax.numpy as jnp
from jax import lax
from jax.experimental import pallas as pl
from jax.experimental.pallas import tpu as pltpu
from jax.sharding import PartitionSpec as P

keep_rate = 0.8
fresh_rate = 1.0 - keep_rate
GROUPS = 4
MESH = pl.DeviceIdType.MESH
F32 = jnp.float32
BF16 = jnp.bfloat16
scope = jax.named_scope


def mul(a, b, dims=(1, 0)):
    return lax.dot_general(a, b, (((dims[0],), (dims[1],)), ((), ())), preferred_element_type=F32)


def wait_bytes(ref, sem):
    pltpu.make_async_copy(ref, ref, sem).wait()


def kernel(
    n_dp, n_mp, blocks, row,
    plan, grad, fac, root, fresh, fac_out, plan_s,
    own_g, in_g, fac_v, pieces, full_x, rest, fifth, fac_b, summed, gram_b, out_v, detour,
    load_sem, grad_send, grad_recv, gram_send, gram_recv, root_send, root_recv, out_send, out_recv, detour_send, detour_recv, ready, above,
):
    d = lax.axis_index("dp")
    me = lax.axis_index("mp")
    bs = fac.shape[-1]
    high = bs // n_mp
    half = n_mp // 2
    hb = bs // 2
    wide = bs // GROUPS
    levels = n_mp // row
    level = me // row
    at = me % row
    band = row // 2
    upper_band = at >= band
    start = me - at % band
    side = me // half
    away = 1 - side
    near_cols = pl.ds(pl.multiple_of(side * hb, hb), hb)
    far_cols = pl.ds(pl.multiple_of(away * hb, hb), hb)
    far_first = pl.ds(pl.multiple_of(away * hb, hb), hb // 2)
    far_second = pl.ds(pl.multiple_of(away * hb + hb // 2, hb // 2), hb // 2)
    near_pieces = pl.ds(side * half, half)
    far_pieces = pl.ds(away * half, half)
    parity = me % 2
    collects = d % 2 == parity
    partner = d + 1 - 2 * (d % 2)

    loads = [
        pltpu.make_async_copy(root.at[me], pieces.at[me], load_sem.at[0]),
        pltpu.make_async_copy(fac, fac_v, load_sem.at[1]),
        pltpu.make_async_copy(plan, plan_s, load_sem.at[2]),
        pltpu.make_async_copy(grad.at[d // 2], own_g, load_sem.at[3]),
    ]

    def signal(sem, dp, mp):
        pl.semaphore_signal(sem, inc=1, device_id=(dp, mp), device_id_type=MESH)

    def strip(ref, c, by_cols):
        cut = pl.ds(c * wide, wide)
        return ref.at[:, cut] if by_cols else ref.at[cut, :]

    def strips(ref, c, by_cols):
        cut = pl.ds(c * wide, wide)
        return ref.at[:, :, cut] if by_cols else ref.at[:, cut, :]

    def by_parity(act):
        @pl.when(parity == 0)
        def _():
            act(True)

        @pl.when(parity == 1)
        def _():
            act(False)

    def send_grads(by_cols):
        for c in range(GROUPS):
            for k in range(blocks):
                to = 2 * k + parity

                @pl.when(to != d)
                def _():
                    pltpu.make_async_remote_copy(
                        src_ref=strip(grad.at[k], c, by_cols),
                        dst_ref=strip(in_g.at[(d - to + n_dp) % n_dp - 1], c, by_cols),
                        send_sem=grad_send.at[c // (GROUPS - 1)], recv_sem=grad_recv.at[c],
                        device_id=(to, me), device_id_type=MESH,
                    ).start()

    with scope("BARRIER"):
        barrier = pltpu.get_barrier_semaphore()
        odd_sender = jnp.logical_and(jnp.logical_not(collects), d % 2 == 1)

        @pl.when(collects)
        def _():
            for i in range(1, n_dp):
                signal(barrier, (d + i) % n_dp, me)

        @pl.when(odd_sender)
        def _():
            pl.semaphore_wait(barrier, blocks)
            send_grads(True)

        def greet(first):
            for i in range(band // 2):
                t = first + 2 * i + d % 2

                @pl.when(t != me)
                def _():
                    signal(barrier, d, t)

        for k in range(levels):
            @pl.when(level + k < levels)
            def _():
                greet(start + k * row)

                @pl.when(jnp.logical_not(upper_band))
                def _():
                    greet(start + k * row + band)

        @pl.when(collects)
        def _():
            loads[3].start()

        known = blocks - 1 + band - 1 + level * band + jnp.where(upper_band, (level + 1) * band, 0)

        @pl.when(jnp.logical_and(jnp.logical_not(collects), d % 2 == 0))
        def _():
            pl.semaphore_wait(barrier, blocks)
            send_grads(False)

        @pl.when(collects)
        def _():
            pl.semaphore_wait(barrier, known)
            if blocks > 1:
                by_parity(send_grads)
            signal(ready, d, me + 1 - 2 * parity)

        @pl.when(jnp.logical_and(upper_band, collects))
        def _():
            for k in range(levels):
                @pl.when(level >= k)
                def _():
                    pair = me - at % 2 - k * row
                    for i in range(2):
                        signal(above.at[k], d, pair - band + i)
                        if k:
                            signal(above.at[k], d, pair + i)

    def root_far(t):
        base = side * hb
        upper = me % half < half // 2

        def copy(start, size):
            cols = pl.ds(pl.multiple_of(start, hb // 2), size)
            pltpu.make_async_remote_copy(
                src_ref=root.at[t, :, cols], dst_ref=pieces.at[me, :, cols],
                send_sem=root_send, recv_sem=root_recv, device_id=(d, t), device_id_type=MESH,
            ).start()

        @pl.when(upper)
        def _():
            copy(base, hb)

        @pl.when(jnp.logical_not(upper))
        def _():
            copy(base + hb // 2, hb // 2)

    def root_near(t):
        pltpu.make_async_remote_copy(
            src_ref=root.at[t], dst_ref=pieces.at[me],
            send_sem=root_send, recv_sem=root_recv, device_id=(d, t), device_id_type=MESH,
        ).start()

    def send_roots(to, odd):
        for j in range(band // 2):
            t = to + (at // 2 * 2 + 2 * j) % band + odd
            close = t // half == side

            @pl.when(jnp.logical_not(close))
            def _():
                root_far(t)

            @pl.when(jnp.logical_and(close, t != me))
            def _():
                root_near(t)

    def each_level(odd, meet):
        for k in reversed(range(levels)):
            @pl.when(level >= k)
            def _():
                send_roots((level - k) * row, odd)

        if meet:
            @pl.when(jnp.logical_not(upper_band))
            def _():
                pl.semaphore_wait(above.at[0], 1)

        for k in reversed(range(levels)):
            @pl.when(level >= k)
            def _():
                send_roots((level - k) * row + band, odd)

        for k in range(1, levels):
            @pl.when(level + k < levels)
            def _():
                if meet:
                    pl.semaphore_wait(above.at[k], 1)
                send_roots((level + k) * row, odd)
                send_roots((level + k) * row + band, odd)

    with scope("ROOTSEND"):
        @pl.when(jnp.logical_not(collects))
        def _():
            pl.semaphore_wait(ready, 1)

        each_level(d % 2, True)
        for load in loads[:3]:
            load.start()

    def take(c, by_cols):
        wait_bytes(strips(in_g, c, by_cols), grad_recv.at[c])
        total = strip(own_g, c, by_cols)[...].astype(F32)
        for i in range(n_dp - 1):
            total += strip(in_g.at[i], c, by_cols)[...].astype(F32)
        strip(summed, c, by_cols)[...] = total.astype(BF16)

    def make_row(c, by_cols):
        new = strip(summed, c, by_cols)[...]
        so_far = pl.ds(0, (c + 1) * wide)
        product = mul(new, summed[:, so_far], (0, 0)) if by_cols else mul(new, summed[so_far, :], (1, 1))
        gram_b[pl.ds(c * wide, wide), so_far] = (fresh_rate * product).astype(BF16)

    def gram_row(c):
        part = gram_b.at[pl.ds(c * wide, wide), pl.ds(0, (c + 1) * wide)]
        return pltpu.make_async_remote_copy(
            src_ref=part, dst_ref=part, send_sem=gram_send, recv_sem=gram_recv.at[c // (GROUPS - 1)],
            device_id=(partner, me), device_id_type=MESH,
        )

    early = GROUPS // 2
    with scope("EARLY"):
        @pl.when(collects)
        def _():
            loads[3].wait()

            def act(by_cols):
                for c in range(early):
                    take(c, by_cols)
                    make_row(c, by_cols)
                    if c == 0:
                        each_level(1 - d % 2, False)

            by_parity(act)

        @pl.when(jnp.logical_not(collects))
        def _():
            wait_bytes(in_g.at[pl.ds(0, blocks), pl.ds(0, bs - wide), :], grad_send.at[0])
            each_level(1 - d % 2, False)

    with scope("ROOTRECV"):
        loads[0].wait()
        loads[1].wait()
        wait_bytes(pieces.at[pl.ds(0, half - 1 + half * 3 // 8)], root_recv)

    loads[2].wait()
    kept = plan_s[0, me] >= n_mp
    x_rate = jnp.where(kept, 1.0, 1.25)
    step = jnp.where(kept, 0.0, 0.25)

    with scope("ASSEMBLE"):
        near_rows = pieces[near_pieces].astype(F32).reshape(hb, bs).astype(BF16)
        full_x[near_cols, :] = near_rows
        full_x[far_cols, far_cols] = pieces[far_pieces, :, far_cols].astype(F32).reshape(hb, hb).astype(BF16)
        full_x[far_second, far_first] = full_x[far_first, far_second].astype(F32).T.astype(BF16)
        full_x[far_cols, near_cols] = full_x[near_cols, far_cols].astype(F32).T.astype(BF16)

    with scope("CHAIN"):
        x = full_x[...]
        square = mul(x, x).astype(BF16)
        fourth = mul(square, square).astype(BF16)
        fifth[...] = (step * mul(x, fourth)).astype(BF16)

    def send_out(t):
        pltpu.make_async_remote_copy(
            src_ref=out_v.at[t], dst_ref=fresh.at[me],
            send_sem=out_send, recv_sem=out_recv, device_id=(d, t), device_id_type=MESH,
        ).start()

    middle = levels // 2
    even = d % 2 == 0
    hands = jnp.logical_and(jnp.logical_and(collects, even), level == middle)
    helps = jnp.logical_not(jnp.logical_or(collects, even))
    first_hop = jnp.logical_and(helps, level == middle)
    second_hop = jnp.logical_and(helps, level == middle - 1)

    def send_far(t):
        aside = jnp.logical_and(hands, t == me - row)

        @pl.when(aside)
        def _():
            pltpu.make_async_remote_copy(
                src_ref=out_v.at[t], dst_ref=detour,
                send_sem=out_send, recv_sem=detour_recv, device_id=(partner, me), device_id_type=MESH,
            ).start()

        @pl.when(jnp.logical_not(aside))
        def _():
            send_out(t)

    def hand_on(to, dst, sem):
        wait_bytes(detour, detour_recv)
        pltpu.make_async_remote_copy(
            src_ref=detour, dst_ref=dst,
            send_sem=detour_send, recv_sem=sem, device_id=to, device_id_type=MESH,
        ).start()

    def refine(first, count, value):
        rows = pl.ds(pl.multiple_of(first * high, high), count * high)
        out_v[pl.ds(first, count)] = value(rows).reshape(count, high, bs).astype(BF16)

    def give_far(k, value):
        to = away * half + k * row
        refine(to, row, value)
        for j in range(row):
            turn = jnp.where(to == 0, j // band, (j // band + 1 + upper_band.astype(jnp.int32)) % 2)
            send_far(to + turn * band + (at + j) % band)

    def give_near(value):
        refine(side * half, half, value)

        @pl.loop(1, half)
        def _(i):
            send_out(side * half + (me + i) % half)

    def with_factor(rows):
        return x_rate * full_x[rows, :].astype(F32) - mul(fifth[rows, :], fac_b[...])

    @pl.when(collects)
    def _():
        def act(by_cols):
            dims = (1, 1) if by_cols else (0, 0)
            across = (1, 0) if by_cols else (1, 1)
            back = (1, 1) if by_cols else (1, 0)
            last = GROUPS - 1
            first_rows = pl.ds(pl.multiple_of(away * hb, hb), row * high)
            with scope("GRADS"):
                for c in range(early, last):
                    take(c, by_cols)
                    make_row(c, by_cols)
                for c in range(last):
                    gram_row(c).start()
                cut = pl.ds(0, last * wide)
                known = summed[:, cut] if by_cols else summed[cut, :]
                total = keep_rate * fac_v[...] + fresh_rate * mul(known, known, dims)
                fac_out[...] = total
                fac_b[...] = total.astype(BF16)
                rest[first_rows, :] = with_factor(first_rows)
            with scope("GRADLAST"):
                take(last, by_cols)
                new = strip(summed, last, by_cols)[...]
                turned = (fresh_rate * mul(fifth[first_rows, :], new, across)).astype(BF16)
                give_far(0, lambda rows: rest[rows, :] - mul(turned, new, back))
            with scope("ROWLAST"):
                make_row(last, by_cols)
                gram_row(last).start()
            with scope("GIVEFAR"):
                fac_b[...] = (fac_out[...] + fresh_rate * mul(new, new, dims)).astype(BF16)
                for k in range(1, half // row):
                    give_far(k, with_factor)
            with scope("GIVENEAR"):
                give_near(with_factor)
            with scope("FACOUT"):
                fac_out[...] += fresh_rate * mul(new, new, dims)
            wait_bytes(gram_b.at[pl.ds(0, bs * (GROUPS + 1) // (2 * GROUPS))], gram_send)

        by_parity(act)

    @pl.when(jnp.logical_not(collects))
    def _():
        with scope("REST"):
            rest[...] = x_rate * full_x[...].astype(F32) - keep_rate * mul(fifth[...], fac_v[...].astype(BF16))
        def mirror(c):
            rows = pl.ds(c * wide, wide)
            before = pl.ds(0, c * wide)
            gram_b[before, rows] = gram_b[rows, before].astype(F32).T.astype(BF16)

        last = GROUPS - 1
        with scope("GRAMIN"):
            wait_bytes(gram_b.at[pl.ds(0, last * wide), pl.ds(0, bs // 2)], gram_recv.at[0])
            for c in range(1, last):
                mirror(c)

            @pl.when(first_hop)
            def _():
                hand_on((d, me - row), detour, detour_recv)
        with scope("GRAMLAST"):
            gram_row(last).wait_recv()
            mirror(last)

        def with_gram(rows):
            return rest[rows, :] - mul(fifth[rows, :], gram_b[...])

        with scope("GIVEFAR"):
            for k in range(half // row):
                give_far(k, with_gram)
        with scope("GIVENEAR"):
            give_near(with_gram)
        with scope("FACOUT"):
            fac_out[...] = keep_rate * fac_v[...] + gram_b[...].astype(F32)
            wait_bytes(in_g.at[pl.ds(0, blocks), pl.ds(0, wide), :], grad_send.at[1])

            @pl.when(second_hop)
            def _():
                hand_on((partner, me), fresh.at[me + row], out_recv)

            @pl.when(jnp.logical_or(first_hop, second_hop))
            def _():
                wait_bytes(detour, detour_send)

    with scope("SENDS"):
        own_out = pltpu.make_async_copy(out_v.at[me], fresh.at[me], load_sem.at[0])
        own_out.start()
        if blocks > 1:
            @pl.when(collects)
            def _():
                wait_bytes(in_g.at[pl.ds(0, blocks - 1), pl.ds(0, bs - wide), :], grad_send.at[0])
                wait_bytes(in_g.at[pl.ds(0, blocks - 1), pl.ds(0, wide), :], grad_send.at[1])

        @pl.when(me % half < half // 2)
        def _():
            wait_bytes(pieces.at[pl.ds(0, half - 1 + half // 2)], root_send)

        @pl.when(me % half >= half // 2)
        def _():
            wait_bytes(pieces.at[pl.ds(0, half - 1 + half // 4)], root_send)

        own_out.wait()
        wait_bytes(out_v.at[pl.ds(0, n_mp - 1)], out_send)

    with scope("RECV"):
        wait_bytes(fresh.at[pl.ds(0, n_mp - 1)], out_recv)


def write_out(fac_v, fresh_v, fac_out, fresh_out, sem):
    copies = [
        pltpu.make_async_copy(fac_v, fac_out, sem.at[0]),
        pltpu.make_async_copy(fresh_v, fresh_out, sem.at[1]),
    ]
    for copy in copies:
        copy.start()
    for copy in copies:
        copy.wait()


def level_size(n_mp):
    size = 1
    while size * size < n_mp:
        size *= 2
    return size


def local(n_dp, n_mp, grad_parts, factors, root_prev, plan):
    blocks, bs = grad_parts.shape[2], factors.shape[-1]
    high = bs // n_mp
    row = level_size(n_mp)
    wide = bs // GROUPS
    grads = grad_parts.reshape(blocks, bs, bs)
    old = root_prev.reshape(n_mp, high, bs)
    fresh, new_factor = pl.pallas_call(
        functools.partial(kernel, n_dp, n_mp, blocks, row),
        out_shape=(
            pltpu.VMEM((n_mp, high, bs), BF16),
            pltpu.VMEM((bs, bs), F32),
        ),
        in_specs=[pl.BlockSpec(memory_space=pl.ANY)] * 4,
        out_specs=(pl.BlockSpec(memory_space=pltpu.VMEM),) * 2,
        scratch_shapes=[
            pltpu.SMEM(plan.shape, plan.dtype),
            pltpu.VMEM((bs, bs), BF16),
            pltpu.VMEM((n_dp - 1, bs, bs), BF16),
            pltpu.VMEM((bs, bs), F32),
            pltpu.VMEM((n_mp, high, bs), BF16),
            pltpu.VMEM((bs, bs), BF16),
            pltpu.VMEM((bs, bs), F32),
            pltpu.VMEM((bs, bs), BF16),
            pltpu.VMEM((bs, bs), BF16),
            pltpu.VMEM((bs, bs), BF16),
            pltpu.VMEM((bs, bs), BF16),
            pltpu.VMEM((n_mp, high, bs), BF16),
            pltpu.VMEM((high, bs), BF16),
            pltpu.SemaphoreType.DMA((4,)),
            pltpu.SemaphoreType.DMA((2,)),
            pltpu.SemaphoreType.DMA((GROUPS,)),
            pltpu.SemaphoreType.DMA,
            pltpu.SemaphoreType.DMA((2,)),
            pltpu.SemaphoreType.DMA,
            pltpu.SemaphoreType.DMA,
            pltpu.SemaphoreType.DMA,
            pltpu.SemaphoreType.DMA,
            pltpu.SemaphoreType.DMA,
            pltpu.SemaphoreType.DMA,
            pltpu.SemaphoreType.REGULAR,
            pltpu.SemaphoreType.REGULAR((n_mp // row,)),
        ],
        compiler_params=pltpu.CompilerParams(collective_id=0, has_side_effects=True),
        name="refresh",
    )(plan, grads, factors.reshape(bs, bs), old)
    new_factor, fresh = pl.pallas_call(
        write_out,
        out_shape=(
            jax.ShapeDtypeStruct((bs, bs), F32),
            jax.ShapeDtypeStruct((n_mp, high, bs), BF16),
        ),
        in_specs=[pl.BlockSpec(memory_space=pl.ANY)] * 2,
        out_specs=(pl.BlockSpec(memory_space=pl.ANY),) * 2,
        scratch_shapes=[pltpu.SemaphoreType.DMA((2,))],
        compiler_params=pltpu.CompilerParams(vmem_limit_bytes=1 << 20),
        name="write_out",
    )(new_factor, fresh)
    return (new_factor[None, None], fresh.reshape(root_prev.shape))


def solution(mesh):
    return jax.shard_map(
        functools.partial(local, mesh.shape["dp"], mesh.shape["mp"]),
        mesh=mesh,
        in_specs=(
            P("dp", "mp", None, None, None),
            P("mp", "dp", None, None),
            P(None, "dp", "mp", None),
            P("dp", None),
        ),
        out_specs=(P("mp", "dp", None, None), P(None, "dp", "mp", None)),
        check_vma=False,
    )
```

```python
import functools

import jax
import jax.numpy as jnp
from jax import lax
from jax.experimental import pallas as pl
from jax.experimental.pallas import tpu as pltpu
from jax.sharding import PartitionSpec as P

keep_rate = 0.8
fresh_rate = 1.0 - keep_rate
GROUPS = 4
MESH = pl.DeviceIdType.MESH
F32 = jnp.float32
BF16 = jnp.bfloat16
scope = jax.named_scope


def mul(a, b, dims=(1, 0)):
    return lax.dot_general(a, b, (((dims[0],), (dims[1],)), ((), ())), preferred_element_type=F32)


def wait_bytes(ref, sem):
    pltpu.make_async_copy(ref, ref, sem).wait()


def kernel(
    n_dp, n_mp, blocks, row,
    plan, grad, fac, root, fresh, fac_out, plan_s,
    own_g, in_g, fac_v, pieces, full_x, rest, fifth, fac_b, summed, gram_b, out_v, detour,
    load_sem, grad_send, grad_recv, gram_send, gram_recv, root_send, root_recv, out_send, out_recv, detour_send, detour_recv, ready, above,
):
    d = lax.axis_index("dp")
    me = lax.axis_index("mp")
    bs = fac.shape[-1]
    high = bs // n_mp
    half = n_mp // 2
    hb = bs // 2
    wide = bs // GROUPS
    levels = n_mp // row
    level = me // row
    at = me % row
    band = row // 2
    upper_band = at >= band
    start = me - at % band
    side = me // half
    away = 1 - side
    near_cols = pl.ds(pl.multiple_of(side * hb, hb), hb)
    far_cols = pl.ds(pl.multiple_of(away * hb, hb), hb)
    far_first = pl.ds(pl.multiple_of(away * hb, hb), hb // 2)
    far_second = pl.ds(pl.multiple_of(away * hb + hb // 2, hb // 2), hb // 2)
    near_pieces = pl.ds(side * half, half)
    far_pieces = pl.ds(away * half, half)
    parity = me % 2
    collects = d % 2 == parity
    partner = d + 1 - 2 * (d % 2)

    loads = [
        pltpu.make_async_copy(root.at[me], pieces.at[me], load_sem.at[0]),
        pltpu.make_async_copy(fac, fac_v, load_sem.at[1]),
        pltpu.make_async_copy(plan, plan_s, load_sem.at[2]),
        pltpu.make_async_copy(grad.at[d // 2], own_g, load_sem.at[3]),
    ]

    def signal(sem, dp, mp):
        pl.semaphore_signal(sem, inc=1, device_id=(dp, mp), device_id_type=MESH)

    def strip(ref, c, by_cols):
        cut = pl.ds(c * wide, wide)
        return ref.at[:, cut] if by_cols else ref.at[cut, :]

    def strips(ref, c, by_cols):
        cut = pl.ds(c * wide, wide)
        return ref.at[:, :, cut] if by_cols else ref.at[:, cut, :]

    def by_parity(act):
        @pl.when(parity == 0)
        def _():
            act(True)

        @pl.when(parity == 1)
        def _():
            act(False)

    def send_grads(by_cols):
        for c in range(GROUPS):
            for k in range(blocks):
                to = 2 * k + parity

                @pl.when(to != d)
                def _():
                    pltpu.make_async_remote_copy(
                        src_ref=strip(grad.at[k], c, by_cols),
                        dst_ref=strip(in_g.at[(d - to + n_dp) % n_dp - 1], c, by_cols),
                        send_sem=grad_send.at[c // (GROUPS - 1)], recv_sem=grad_recv.at[c],
                        device_id=(to, me), device_id_type=MESH,
                    ).start()

    with scope("BARRIER"):
        barrier = pltpu.get_barrier_semaphore()
        odd_sender = jnp.logical_and(jnp.logical_not(collects), d % 2 == 1)

        @pl.when(collects)
        def _():
            for i in range(1, n_dp):
                signal(barrier, (d + i) % n_dp, me)

        @pl.when(odd_sender)
        def _():
            pl.semaphore_wait(barrier, blocks)
            send_grads(True)

        def greet(first):
            for i in range(band // 2):
                t = first + 2 * i + d % 2

                @pl.when(t != me)
                def _():
                    signal(barrier, d, t)

        for k in range(levels):
            @pl.when(level + k < levels)
            def _():
                greet(start + k * row)

                @pl.when(jnp.logical_not(upper_band))
                def _():
                    greet(start + k * row + band)

        @pl.when(collects)
        def _():
            loads[3].start()

        known = blocks - 1 + band - 1 + level * band + jnp.where(upper_band, (level + 1) * band, 0)

        @pl.when(jnp.logical_and(jnp.logical_not(collects), d % 2 == 0))
        def _():
            pl.semaphore_wait(barrier, blocks)
            send_grads(False)

        @pl.when(collects)
        def _():
            pl.semaphore_wait(barrier, known)
            if blocks > 1:
                by_parity(send_grads)
            signal(ready, d, me + 1 - 2 * parity)

        @pl.when(jnp.logical_and(upper_band, collects))
        def _():
            for k in range(levels):
                @pl.when(level >= k)
                def _():
                    pair = me - at % 2 - k * row
                    for i in range(2):
                        signal(above.at[k], d, pair - band + i)
                        if k:
                            signal(above.at[k], d, pair + i)

    def root_far(t):
        base = side * hb
        upper = me % half < half // 2

        def copy(start, size):
            cols = pl.ds(pl.multiple_of(start, hb // 2), size)
            pltpu.make_async_remote_copy(
                src_ref=root.at[t, :, cols], dst_ref=pieces.at[me, :, cols],
                send_sem=root_send, recv_sem=root_recv, device_id=(d, t), device_id_type=MESH,
            ).start()

        @pl.when(upper)
        def _():
            copy(base, hb)

        @pl.when(jnp.logical_not(upper))
        def _():
            copy(base + hb // 2, hb // 2)

    def root_near(t):
        pltpu.make_async_remote_copy(
            src_ref=root.at[t], dst_ref=pieces.at[me],
            send_sem=root_send, recv_sem=root_recv, device_id=(d, t), device_id_type=MESH,
        ).start()

    def send_roots(to, odd):
        for j in range(band // 2):
            t = to + (at // 2 * 2 + 2 * j) % band + odd
            close = t // half == side

            @pl.when(jnp.logical_not(close))
            def _():
                root_far(t)

            @pl.when(jnp.logical_and(close, t != me))
            def _():
                root_near(t)

    def each_level(odd, meet):
        for k in reversed(range(levels)):
            @pl.when(level >= k)
            def _():
                send_roots((level - k) * row, odd)

        if meet:
            @pl.when(jnp.logical_not(upper_band))
            def _():
                pl.semaphore_wait(above.at[0], 1)

        for k in reversed(range(levels)):
            @pl.when(level >= k)
            def _():
                send_roots((level - k) * row + band, odd)

        for k in range(1, levels):
            @pl.when(level + k < levels)
            def _():
                if meet:
                    pl.semaphore_wait(above.at[k], 1)
                send_roots((level + k) * row, odd)
                send_roots((level + k) * row + band, odd)

    with scope("ROOTSEND"):
        @pl.when(jnp.logical_not(collects))
        def _():
            pl.semaphore_wait(ready, 1)

        each_level(d % 2, True)
        for load in loads[:3]:
            load.start()

    def take(c, by_cols):
        wait_bytes(strips(in_g, c, by_cols), grad_recv.at[c])
        total = strip(own_g, c, by_cols)[...].astype(F32)
        for i in range(n_dp - 1):
            total += strip(in_g.at[i], c, by_cols)[...].astype(F32)
        strip(summed, c, by_cols)[...] = total.astype(BF16)

    def make_row(c, by_cols):
        new = strip(summed, c, by_cols)[...]
        so_far = pl.ds(0, (c + 1) * wide)
        product = mul(new, summed[:, so_far], (0, 0)) if by_cols else mul(new, summed[so_far, :], (1, 1))
        gram_b[pl.ds(c * wide, wide), so_far] = (fresh_rate * product).astype(BF16)

    def gram_row(c):
        part = gram_b.at[pl.ds(c * wide, wide), pl.ds(0, (c + 1) * wide)]
        return pltpu.make_async_remote_copy(
            src_ref=part, dst_ref=part, send_sem=gram_send, recv_sem=gram_recv.at[c // (GROUPS - 1)],
            device_id=(partner, me), device_id_type=MESH,
        )

    early = GROUPS // 2
    with scope("EARLY"):
        @pl.when(collects)
        def _():
            loads[3].wait()

            def act(by_cols):
                for c in range(early):
                    take(c, by_cols)
                    make_row(c, by_cols)
                    if c == 0:
                        each_level(1 - d % 2, False)

            by_parity(act)

        @pl.when(jnp.logical_not(collects))
        def _():
            wait_bytes(in_g.at[pl.ds(0, blocks), pl.ds(0, bs - wide), :], grad_send.at[0])
            each_level(1 - d % 2, False)

    with scope("ROOTRECV"):
        loads[0].wait()
        loads[1].wait()
        wait_bytes(pieces.at[pl.ds(0, half - 1 + half * 3 // 8)], root_recv)

    loads[2].wait()
    kept = plan_s[0, me] >= n_mp
    x_rate = jnp.where(kept, 1.0, 1.25)
    step = jnp.where(kept, 0.0, 0.25)

    with scope("ASSEMBLE"):
        near_rows = pieces[near_pieces].astype(F32).reshape(hb, bs).astype(BF16)
        full_x[near_cols, :] = near_rows
        full_x[far_cols, far_cols] = pieces[far_pieces, :, far_cols].astype(F32).reshape(hb, hb).astype(BF16)
        full_x[far_second, far_first] = full_x[far_first, far_second].astype(F32).T.astype(BF16)
        full_x[far_cols, near_cols] = full_x[near_cols, far_cols].astype(F32).T.astype(BF16)

    with scope("CHAIN"):
        x = full_x[...]
        square = mul(x, x).astype(BF16)
        fourth = mul(square, square).astype(BF16)
        fifth[...] = (step * mul(x, fourth)).astype(BF16)

    def send_out(t):
        pltpu.make_async_remote_copy(
            src_ref=out_v.at[t], dst_ref=fresh.at[me],
            send_sem=out_send, recv_sem=out_recv, device_id=(d, t), device_id_type=MESH,
        ).start()

    middle = levels // 2
    even = d % 2 == 0
    hands = jnp.logical_and(jnp.logical_and(collects, even), level == middle)
    helps = jnp.logical_not(jnp.logical_or(collects, even))
    first_hop = jnp.logical_and(helps, level == middle)
    second_hop = jnp.logical_and(helps, level == middle - 1)

    def send_far(t):
        aside = jnp.logical_and(hands, t == me - row)

        @pl.when(aside)
        def _():
            pltpu.make_async_remote_copy(
                src_ref=out_v.at[t], dst_ref=detour,
                send_sem=out_send, recv_sem=detour_recv, device_id=(partner, me), device_id_type=MESH,
            ).start()

        @pl.when(jnp.logical_not(aside))
        def _():
            send_out(t)

    def hand_on(to, dst, sem):
        wait_bytes(detour, detour_recv)
        pltpu.make_async_remote_copy(
            src_ref=detour, dst_ref=dst,
            send_sem=detour_send, recv_sem=sem, device_id=to, device_id_type=MESH,
        ).start()

    def refine(first, count, value):
        rows = pl.ds(pl.multiple_of(first * high, high), count * high)
        out_v[pl.ds(first, count)] = value(rows).reshape(count, high, bs).astype(BF16)

    def give_far(k, value):
        to = away * half + k * row
        refine(to, row, value)
        for j in range(row):
            turn = jnp.where(to == 0, j // band, (j // band + 1 + upper_band.astype(jnp.int32)) % 2)
            send_far(to + turn * band + (at + j) % band)

    def give_near(value):
        refine(side * half, half, value)

        @pl.loop(1, half)
        def _(i):
            send_out(side * half + (me + i) % half)

    def with_factor(rows):
        return x_rate * full_x[rows, :].astype(F32) - mul(fifth[rows, :], fac_b[...])

    @pl.when(collects)
    def _():
        def act(by_cols):
            dims = (1, 1) if by_cols else (0, 0)
            across = (1, 0) if by_cols else (1, 1)
            back = (1, 1) if by_cols else (1, 0)
            last = GROUPS - 1
            first_rows = pl.ds(pl.multiple_of(away * hb, hb), row * high)
            if by_cols:
                with scope("GRADS"):
                    for c in range(early, last):
                        take(c, by_cols)
                        make_row(c, by_cols)
                    for c in range(last):
                        gram_row(c).start()
                    known = summed[:, pl.ds(0, last * wide)]
                    total = keep_rate * fac_v[...] + fresh_rate * mul(known, known, dims)
                    fac_out[...] = total
                    fac_b[...] = total.astype(BF16)
                    rest[first_rows, :] = with_factor(first_rows)
                with scope("GRADLAST"):
                    take(last, by_cols)
                    new = strip(summed, last, by_cols)[...]
                    turned = (fresh_rate * mul(fifth[first_rows, :], new, across)).astype(BF16)
                    give_far(0, lambda rows: rest[rows, :] - mul(turned, new, back))
                with scope("ROWLAST"):
                    make_row(last, by_cols)
                    gram_row(last).start()
                with scope("GIVEFAR"):
                    fac_b[...] = (fac_out[...] + fresh_rate * mul(new, new, dims)).astype(BF16)
            else:
                with scope("GRADS"):
                    for c in range(early):
                        gram_row(c).start()
                    for c in range(early, GROUPS):
                        take(c, by_cols)
                    whole = summed[...]
                    total = keep_rate * fac_v[...] + fresh_rate * mul(whole, whole, dims)
                    fac_out[...] = total
                    fac_b[...] = total.astype(BF16)
                with scope("GRADLAST"):
                    give_far(0, with_factor)
                with scope("ROWLAST"):
                    for c in range(early, GROUPS):
                        make_row(c, by_cols)
                        gram_row(c).start()
            with scope("GIVEFAR"):
                for k in range(1, half // row):
                    give_far(k, with_factor)
            with scope("GIVENEAR"):
                give_near(with_factor)
            if by_cols:
                with scope("FACOUT"):
                    fac_out[...] += fresh_rate * mul(new, new, dims)
            wait_bytes(gram_b.at[pl.ds(0, bs * (GROUPS + 1) // (2 * GROUPS))], gram_send)

        by_parity(act)

    @pl.when(jnp.logical_not(collects))
    def _():
        with scope("REST"):
            rest[...] = x_rate * full_x[...].astype(F32) - keep_rate * mul(fifth[...], fac_v[...].astype(BF16))
        def mirror(c):
            rows = pl.ds(c * wide, wide)
            before = pl.ds(0, c * wide)
            gram_b[before, rows] = gram_b[rows, before].astype(F32).T.astype(BF16)

        last = GROUPS - 1
        with scope("GRAMIN"):
            wait_bytes(gram_b.at[pl.ds(0, last * wide), pl.ds(0, bs // 2)], gram_recv.at[0])
            for c in range(1, last):
                mirror(c)

            @pl.when(first_hop)
            def _():
                hand_on((d, me - row), detour, detour_recv)
        with scope("GRAMLAST"):
            gram_row(last).wait_recv()
            mirror(last)

        def with_gram(rows):
            return rest[rows, :] - mul(fifth[rows, :], gram_b[...])

        with scope("GIVEFAR"):
            for k in range(half // row):
                give_far(k, with_gram)
        with scope("GIVENEAR"):
            give_near(with_gram)
        with scope("FACOUT"):
            fac_out[...] = keep_rate * fac_v[...] + gram_b[...].astype(F32)
            wait_bytes(in_g.at[pl.ds(0, blocks), pl.ds(0, wide), :], grad_send.at[1])

            @pl.when(second_hop)
            def _():
                hand_on((partner, me), fresh.at[me + row], out_recv)

            @pl.when(jnp.logical_or(first_hop, second_hop))
            def _():
                wait_bytes(detour, detour_send)

    with scope("SENDS"):
        own_out = pltpu.make_async_copy(out_v.at[me], fresh.at[me], load_sem.at[0])
        own_out.start()
        if blocks > 1:
            @pl.when(collects)
            def _():
                wait_bytes(in_g.at[pl.ds(0, blocks - 1), pl.ds(0, bs - wide), :], grad_send.at[0])
                wait_bytes(in_g.at[pl.ds(0, blocks - 1), pl.ds(0, wide), :], grad_send.at[1])

        @pl.when(me % half < half // 2)
        def _():
            wait_bytes(pieces.at[pl.ds(0, half - 1 + half // 2)], root_send)

        @pl.when(me % half >= half // 2)
        def _():
            wait_bytes(pieces.at[pl.ds(0, half - 1 + half // 4)], root_send)

        own_out.wait()
        wait_bytes(out_v.at[pl.ds(0, n_mp - 1)], out_send)

    with scope("RECV"):
        wait_bytes(fresh.at[pl.ds(0, n_mp - 1)], out_recv)


def write_out(fac_v, fresh_v, fac_out, fresh_out, sem):
    copies = [
        pltpu.make_async_copy(fac_v, fac_out, sem.at[0]),
        pltpu.make_async_copy(fresh_v, fresh_out, sem.at[1]),
    ]
    for copy in copies:
        copy.start()
    for copy in copies:
        copy.wait()


def level_size(n_mp):
    size = 1
    while size * size < n_mp:
        size *= 2
    return size


def local(n_dp, n_mp, grad_parts, factors, root_prev, plan):
    blocks, bs = grad_parts.shape[2], factors.shape[-1]
    high = bs // n_mp
    row = level_size(n_mp)
    wide = bs // GROUPS
    grads = grad_parts.reshape(blocks, bs, bs)
    old = root_prev.reshape(n_mp, high, bs)
    fresh, new_factor = pl.pallas_call(
        functools.partial(kernel, n_dp, n_mp, blocks, row),
        out_shape=(
            pltpu.VMEM((n_mp, high, bs), BF16),
            pltpu.VMEM((bs, bs), F32),
        ),
        in_specs=[pl.BlockSpec(memory_space=pl.ANY)] * 4,
        out_specs=(pl.BlockSpec(memory_space=pltpu.VMEM),) * 2,
        scratch_shapes=[
            pltpu.SMEM(plan.shape, plan.dtype),
            pltpu.VMEM((bs, bs), BF16),
            pltpu.VMEM((n_dp - 1, bs, bs), BF16),
            pltpu.VMEM((bs, bs), F32),
            pltpu.VMEM((n_mp, high, bs), BF16),
            pltpu.VMEM((bs, bs), BF16),
            pltpu.VMEM((bs, bs), F32),
            pltpu.VMEM((bs, bs), BF16),
            pltpu.VMEM((bs, bs), BF16),
            pltpu.VMEM((bs, bs), BF16),
            pltpu.VMEM((bs, bs), BF16),
            pltpu.VMEM((n_mp, high, bs), BF16),
            pltpu.VMEM((high, bs), BF16),
            pltpu.SemaphoreType.DMA((4,)),
            pltpu.SemaphoreType.DMA((2,)),
            pltpu.SemaphoreType.DMA((GROUPS,)),
            pltpu.SemaphoreType.DMA,
            pltpu.SemaphoreType.DMA((2,)),
            pltpu.SemaphoreType.DMA,
            pltpu.SemaphoreType.DMA,
            pltpu.SemaphoreType.DMA,
            pltpu.SemaphoreType.DMA,
            pltpu.SemaphoreType.DMA,
            pltpu.SemaphoreType.DMA,
            pltpu.SemaphoreType.REGULAR,
            pltpu.SemaphoreType.REGULAR((n_mp // row,)),
        ],
        compiler_params=pltpu.CompilerParams(collective_id=0, has_side_effects=True),
        name="refresh",
    )(plan, grads, factors.reshape(bs, bs), old)
    new_factor, fresh = pl.pallas_call(
        write_out,
        out_shape=(
            jax.ShapeDtypeStruct((bs, bs), F32),
            jax.ShapeDtypeStruct((n_mp, high, bs), BF16),
        ),
        in_specs=[pl.BlockSpec(memory_space=pl.ANY)] * 2,
        out_specs=(pl.BlockSpec(memory_space=pl.ANY),) * 2,
        scratch_shapes=[pltpu.SemaphoreType.DMA((2,))],
        compiler_params=pltpu.CompilerParams(vmem_limit_bytes=1 << 20),
        name="write_out",
    )(new_factor, fresh)
    return (new_factor[None, None], fresh.reshape(root_prev.shape))


def solution(mesh):
    return jax.shard_map(
        functools.partial(local, mesh.shape["dp"], mesh.shape["mp"]),
        mesh=mesh,
        in_specs=(
            P("dp", "mp", None, None, None),
            P("mp", "dp", None, None),
            P(None, "dp", "mp", None),
            P("dp", None),
        ),
        out_specs=(P("mp", "dp", None, None), P(None, "dp", "mp", None)),
        check_vma=False,
    )
```

```python
import functools

import jax
import jax.numpy as jnp
from jax import lax
from jax.experimental import pallas as pl
from jax.experimental.pallas import tpu as pltpu
from jax.sharding import PartitionSpec as P

keep_rate = 0.8
fresh_rate = 1.0 - keep_rate
GROUPS = 4
MESH = pl.DeviceIdType.MESH
F32 = jnp.float32
BF16 = jnp.bfloat16
scope = jax.named_scope


def mul(a, b, dims=(1, 0)):
    return lax.dot_general(a, b, (((dims[0],), (dims[1],)), ((), ())), preferred_element_type=F32)


def wait_bytes(ref, sem):
    pltpu.make_async_copy(ref, ref, sem).wait()


def kernel(
    n_dp, n_mp, blocks, row,
    plan, grad, fac, root, fresh, fac_out, plan_s,
    own_g, in_g, fac_v, pieces, full_x, rest, fifth, fac_b, summed, gram_b, out_v, detour,
    load_sem, grad_send, grad_recv, gram_send, gram_recv, root_send, root_recv, out_send, out_recv, detour_send, detour_recv, ready, above,
):
    d = lax.axis_index("dp")
    me = lax.axis_index("mp")
    bs = fac.shape[-1]
    high = bs // n_mp
    half = n_mp // 2
    hb = bs // 2
    wide = bs // GROUPS
    levels = n_mp // row
    level = me // row
    at = me % row
    band = row // 2
    upper_band = at >= band
    start = me - at % band
    side = me // half
    away = 1 - side
    near_cols = pl.ds(pl.multiple_of(side * hb, hb), hb)
    far_cols = pl.ds(pl.multiple_of(away * hb, hb), hb)
    far_first = pl.ds(pl.multiple_of(away * hb, hb), hb // 2)
    far_second = pl.ds(pl.multiple_of(away * hb + hb // 2, hb // 2), hb // 2)
    near_pieces = pl.ds(side * half, half)
    far_pieces = pl.ds(away * half, half)
    parity = me % 2
    collects = d % 2 == parity
    partner = d + 1 - 2 * (d % 2)

    loads = [
        pltpu.make_async_copy(root.at[me], pieces.at[me], load_sem.at[0]),
        pltpu.make_async_copy(fac, fac_v, load_sem.at[1]),
        pltpu.make_async_copy(plan, plan_s, load_sem.at[2]),
        pltpu.make_async_copy(grad.at[d // 2], own_g, load_sem.at[3]),
    ]

    def signal(sem, dp, mp):
        pl.semaphore_signal(sem, inc=1, device_id=(dp, mp), device_id_type=MESH)

    def strip(ref, c, by_cols):
        cut = pl.ds(c * wide, wide)
        return ref.at[:, cut] if by_cols else ref.at[cut, :]

    def strips(ref, c, by_cols):
        cut = pl.ds(c * wide, wide)
        return ref.at[:, :, cut] if by_cols else ref.at[:, cut, :]

    def by_parity(act):
        @pl.when(parity == 0)
        def _():
            act(True)

        @pl.when(parity == 1)
        def _():
            act(False)

    def send_grads(by_cols):
        for c in range(GROUPS):
            for k in range(blocks):
                to = 2 * k + parity

                @pl.when(to != d)
                def _():
                    pltpu.make_async_remote_copy(
                        src_ref=strip(grad.at[k], c, by_cols),
                        dst_ref=strip(in_g.at[(d - to + n_dp) % n_dp - 1], c, by_cols),
                        send_sem=grad_send.at[c // (GROUPS - 1)], recv_sem=grad_recv.at[c],
                        device_id=(to, me), device_id_type=MESH,
                    ).start()

    with scope("BARRIER"):
        barrier = pltpu.get_barrier_semaphore()
        odd_sender = jnp.logical_and(jnp.logical_not(collects), d % 2 == 1)

        @pl.when(collects)
        def _():
            for i in range(1, n_dp):
                signal(barrier, (d + i) % n_dp, me)

        @pl.when(odd_sender)
        def _():
            pl.semaphore_wait(barrier, blocks)
            send_grads(True)

        def greet(first):
            for i in range(band // 2):
                t = first + 2 * i + d % 2

                @pl.when(t != me)
                def _():
                    signal(barrier, d, t)

        for k in range(levels):
            @pl.when(level + k < levels)
            def _():
                greet(start + k * row)

                @pl.when(jnp.logical_not(upper_band))
                def _():
                    greet(start + k * row + band)

        @pl.when(collects)
        def _():
            loads[3].start()

        known = blocks - 1 + band - 1 + level * band + jnp.where(upper_band, (level + 1) * band, 0)

        @pl.when(jnp.logical_and(jnp.logical_not(collects), d % 2 == 0))
        def _():
            pl.semaphore_wait(barrier, blocks)
            send_grads(False)

        @pl.when(collects)
        def _():
            pl.semaphore_wait(barrier, known)
            if blocks > 1:
                by_parity(send_grads)
            signal(ready, d, me + 1 - 2 * parity)

        @pl.when(jnp.logical_and(upper_band, collects))
        def _():
            for k in range(levels):
                @pl.when(level >= k)
                def _():
                    pair = me - at % 2 - k * row
                    for i in range(2):
                        signal(above.at[k], d, pair - band + i)
                        if k:
                            signal(above.at[k], d, pair + i)

    def root_far(t):
        base = side * hb
        upper = me % half < half // 2

        def copy(start, size):
            cols = pl.ds(pl.multiple_of(start, hb // 2), size)
            pltpu.make_async_remote_copy(
                src_ref=root.at[t, :, cols], dst_ref=pieces.at[me, :, cols],
                send_sem=root_send, recv_sem=root_recv, device_id=(d, t), device_id_type=MESH,
            ).start()

        @pl.when(upper)
        def _():
            copy(base, hb)

        @pl.when(jnp.logical_not(upper))
        def _():
            copy(base + hb // 2, hb // 2)

    def root_near(t):
        pltpu.make_async_remote_copy(
            src_ref=root.at[t], dst_ref=pieces.at[me],
            send_sem=root_send, recv_sem=root_recv, device_id=(d, t), device_id_type=MESH,
        ).start()

    def send_roots(to, odd):
        for j in range(band // 2):
            t = to + (at // 2 * 2 + 2 * j) % band + odd
            close = t // half == side

            @pl.when(jnp.logical_not(close))
            def _():
                root_far(t)

            @pl.when(jnp.logical_and(close, t != me))
            def _():
                root_near(t)

    def each_level(odd, meet):
        for k in reversed(range(levels)):
            @pl.when(level >= k)
            def _():
                send_roots((level - k) * row, odd)

        if meet:
            @pl.when(jnp.logical_not(upper_band))
            def _():
                pl.semaphore_wait(above.at[0], 1)

        for k in reversed(range(levels)):
            @pl.when(level >= k)
            def _():
                send_roots((level - k) * row + band, odd)

        for k in range(1, levels):
            @pl.when(level + k < levels)
            def _():
                if meet:
                    pl.semaphore_wait(above.at[k], 1)
                send_roots((level + k) * row, odd)
                send_roots((level + k) * row + band, odd)

    with scope("ROOTSEND"):
        @pl.when(jnp.logical_not(collects))
        def _():
            pl.semaphore_wait(ready, 1)

        each_level(d % 2, True)
        for load in loads[:3]:
            load.start()

    def take(c, by_cols):
        wait_bytes(strips(in_g, c, by_cols), grad_recv.at[c])
        total = strip(own_g, c, by_cols)[...].astype(F32)
        for i in range(n_dp - 1):
            total += strip(in_g.at[i], c, by_cols)[...].astype(F32)
        strip(summed, c, by_cols)[...] = total.astype(BF16)

    def make_row(c, by_cols):
        new = strip(summed, c, by_cols)[...]
        so_far = pl.ds(0, (c + 1) * wide)
        product = mul(new, summed[:, so_far], (0, 0)) if by_cols else mul(new, summed[so_far, :], (1, 1))
        gram_b[pl.ds(c * wide, wide), so_far] = (fresh_rate * product).astype(BF16)

    def gram_row(c):
        part = gram_b.at[pl.ds(c * wide, wide), pl.ds(0, (c + 1) * wide)]
        return pltpu.make_async_remote_copy(
            src_ref=part, dst_ref=part, send_sem=gram_send, recv_sem=gram_recv.at[c // (GROUPS - 1)],
            device_id=(partner, me), device_id_type=MESH,
        )

    early = GROUPS // 2
    with scope("EARLY"):
        @pl.when(collects)
        def _():
            loads[3].wait()

            def act(by_cols):
                for c in range(early):
                    take(c, by_cols)
                    make_row(c, by_cols)
                    if c == 0:
                        each_level(1 - d % 2, False)

            by_parity(act)

        @pl.when(jnp.logical_not(collects))
        def _():
            wait_bytes(in_g.at[pl.ds(0, blocks), pl.ds(0, bs - wide), :], grad_send.at[0])
            each_level(1 - d % 2, False)

    with scope("ROOTRECV"):
        loads[0].wait()
        loads[1].wait()
        wait_bytes(pieces.at[pl.ds(0, half - 1 + half * 3 // 8)], root_recv)

    loads[2].wait()
    kept = plan_s[0, me] >= n_mp
    x_rate = jnp.where(kept, 1.0, 1.25)
    step = jnp.where(kept, 0.0, 0.25)

    with scope("ASSEMBLE"):
        near_rows = pieces[near_pieces].astype(F32).reshape(hb, bs).astype(BF16)
        full_x[near_cols, :] = near_rows
        full_x[far_cols, far_cols] = pieces[far_pieces, :, far_cols].astype(F32).reshape(hb, hb).astype(BF16)
        full_x[far_second, far_first] = full_x[far_first, far_second].astype(F32).T.astype(BF16)
        full_x[far_cols, near_cols] = full_x[near_cols, far_cols].astype(F32).T.astype(BF16)

    with scope("CHAIN"):
        x = full_x[...]
        square = mul(x, x).astype(BF16)
        fourth = mul(square, square).astype(BF16)
        fifth[...] = (step * mul(x, fourth)).astype(BF16)

    def send_out(t):
        pltpu.make_async_remote_copy(
            src_ref=out_v.at[t], dst_ref=fresh.at[me],
            send_sem=out_send, recv_sem=out_recv, device_id=(d, t), device_id_type=MESH,
        ).start()

    middle = levels // 2
    even = d % 2 == 0
    hands = jnp.logical_and(jnp.logical_and(collects, even), level == middle)
    helps = jnp.logical_not(jnp.logical_or(collects, even))
    first_hop = jnp.logical_and(helps, level == middle)
    second_hop = jnp.logical_and(helps, level == middle - 1)

    def send_far(t):
        aside = jnp.logical_and(hands, t == me - row)

        @pl.when(aside)
        def _():
            pltpu.make_async_remote_copy(
                src_ref=out_v.at[t], dst_ref=detour,
                send_sem=out_send, recv_sem=detour_recv, device_id=(partner, me), device_id_type=MESH,
            ).start()

        @pl.when(jnp.logical_not(aside))
        def _():
            send_out(t)

    def hand_on(to, dst, sem):
        wait_bytes(detour, detour_recv)
        pltpu.make_async_remote_copy(
            src_ref=detour, dst_ref=dst,
            send_sem=detour_send, recv_sem=sem, device_id=to, device_id_type=MESH,
        ).start()

    def refine(first, count, value):
        rows = pl.ds(pl.multiple_of(first * high, high), count * high)
        out_v[pl.ds(first, count)] = value(rows).reshape(count, high, bs).astype(BF16)

    def give_far(k, value):
        to = away * half + k * row
        refine(to, row, value)
        for j in range(row):
            turn = jnp.where(to == 0, j // band, (j // band + 1 + upper_band.astype(jnp.int32)) % 2)
            send_far(to + turn * band + j % band)

    def give_near(value):
        refine(side * half, half, value)

        @pl.loop(1, half)
        def _(i):
            send_out(side * half + (me + i) % half)

    def with_factor(rows):
        return x_rate * full_x[rows, :].astype(F32) - mul(fifth[rows, :], fac_b[...])

    @pl.when(collects)
    def _():
        def act(by_cols):
            dims = (1, 1) if by_cols else (0, 0)
            across = (1, 0) if by_cols else (1, 1)
            back = (1, 1) if by_cols else (1, 0)
            last = GROUPS - 1
            first_rows = pl.ds(pl.multiple_of(away * hb, hb), row * high)
            if by_cols:
                with scope("GRADS"):
                    for c in range(early, last):
                        take(c, by_cols)
                        make_row(c, by_cols)
                    for c in range(last):
                        gram_row(c).start()
                    known = summed[:, pl.ds(0, last * wide)]
                    total = keep_rate * fac_v[...] + fresh_rate * mul(known, known, dims)
                    fac_out[...] = total
                    fac_b[...] = total.astype(BF16)
                    rest[first_rows, :] = with_factor(first_rows)
                with scope("GRADLAST"):
                    take(last, by_cols)
                    new = strip(summed, last, by_cols)[...]
                    turned = (fresh_rate * mul(fifth[first_rows, :], new, across)).astype(BF16)
                    give_far(0, lambda rows: rest[rows, :] - mul(turned, new, back))
                with scope("ROWLAST"):
                    make_row(last, by_cols)
                    gram_row(last).start()
                with scope("GIVEFAR"):
                    fac_b[...] = (fac_out[...] + fresh_rate * mul(new, new, dims)).astype(BF16)
            else:
                with scope("GRADS"):
                    for c in range(early):
                        gram_row(c).start()
                    for c in range(early, GROUPS):
                        take(c, by_cols)
                    whole = summed[...]
                    total = keep_rate * fac_v[...] + fresh_rate * mul(whole, whole, dims)
                    fac_out[...] = total
                    fac_b[...] = total.astype(BF16)
                with scope("GRADLAST"):
                    give_far(0, with_factor)
                with scope("ROWLAST"):
                    for c in range(early, GROUPS):
                        make_row(c, by_cols)
                        gram_row(c).start()
            with scope("GIVEFAR"):
                for k in range(1, half // row):
                    give_far(k, with_factor)
            with scope("GIVENEAR"):
                give_near(with_factor)
            if by_cols:
                with scope("FACOUT"):
                    fac_out[...] += fresh_rate * mul(new, new, dims)
            wait_bytes(gram_b.at[pl.ds(0, bs * (GROUPS + 1) // (2 * GROUPS))], gram_send)

        by_parity(act)

    @pl.when(jnp.logical_not(collects))
    def _():
        with scope("REST"):
            rest[...] = x_rate * full_x[...].astype(F32) - keep_rate * mul(fifth[...], fac_v[...].astype(BF16))
        def mirror(c):
            rows = pl.ds(c * wide, wide)
            before = pl.ds(0, c * wide)
            gram_b[before, rows] = gram_b[rows, before].astype(F32).T.astype(BF16)

        last = GROUPS - 1
        with scope("GRAMIN"):
            wait_bytes(gram_b.at[pl.ds(0, last * wide), pl.ds(0, bs // 2)], gram_recv.at[0])
            for c in range(1, last):
                mirror(c)

            @pl.when(first_hop)
            def _():
                hand_on((d, me - row), detour, detour_recv)
        with scope("GRAMLAST"):
            gram_row(last).wait_recv()
            mirror(last)

        def with_gram(rows):
            return rest[rows, :] - mul(fifth[rows, :], gram_b[...])

        with scope("GIVEFAR"):
            for k in range(half // row):
                give_far(k, with_gram)
        with scope("GIVENEAR"):
            give_near(with_gram)
        with scope("FACOUT"):
            fac_out[...] = keep_rate * fac_v[...] + gram_b[...].astype(F32)
            wait_bytes(in_g.at[pl.ds(0, blocks), pl.ds(0, wide), :], grad_send.at[1])

            @pl.when(second_hop)
            def _():
                hand_on((partner, me), fresh.at[me + row], out_recv)

            @pl.when(jnp.logical_or(first_hop, second_hop))
            def _():
                wait_bytes(detour, detour_send)

    with scope("SENDS"):
        own_out = pltpu.make_async_copy(out_v.at[me], fresh.at[me], load_sem.at[0])
        own_out.start()
        if blocks > 1:
            @pl.when(collects)
            def _():
                wait_bytes(in_g.at[pl.ds(0, blocks - 1), pl.ds(0, bs - wide), :], grad_send.at[0])
                wait_bytes(in_g.at[pl.ds(0, blocks - 1), pl.ds(0, wide), :], grad_send.at[1])

        @pl.when(me % half < half // 2)
        def _():
            wait_bytes(pieces.at[pl.ds(0, half - 1 + half // 2)], root_send)

        @pl.when(me % half >= half // 2)
        def _():
            wait_bytes(pieces.at[pl.ds(0, half - 1 + half // 4)], root_send)

        own_out.wait()
        wait_bytes(out_v.at[pl.ds(0, n_mp - 1)], out_send)

    with scope("RECV"):
        wait_bytes(fresh.at[pl.ds(0, n_mp - 1)], out_recv)


def write_out(fac_v, fresh_v, fac_out, fresh_out, sem):
    copies = [
        pltpu.make_async_copy(fac_v, fac_out, sem.at[0]),
        pltpu.make_async_copy(fresh_v, fresh_out, sem.at[1]),
    ]
    for copy in copies:
        copy.start()
    for copy in copies:
        copy.wait()


def level_size(n_mp):
    size = 1
    while size * size < n_mp:
        size *= 2
    return size


def local(n_dp, n_mp, grad_parts, factors, root_prev, plan):
    blocks, bs = grad_parts.shape[2], factors.shape[-1]
    high = bs // n_mp
    row = level_size(n_mp)
    wide = bs // GROUPS
    grads = grad_parts.reshape(blocks, bs, bs)
    old = root_prev.reshape(n_mp, high, bs)
    fresh, new_factor = pl.pallas_call(
        functools.partial(kernel, n_dp, n_mp, blocks, row),
        out_shape=(
            pltpu.VMEM((n_mp, high, bs), BF16),
            pltpu.VMEM((bs, bs), F32),
        ),
        in_specs=[pl.BlockSpec(memory_space=pl.ANY)] * 4,
        out_specs=(pl.BlockSpec(memory_space=pltpu.VMEM),) * 2,
        scratch_shapes=[
            pltpu.SMEM(plan.shape, plan.dtype),
            pltpu.VMEM((bs, bs), BF16),
            pltpu.VMEM((n_dp - 1, bs, bs), BF16),
            pltpu.VMEM((bs, bs), F32),
            pltpu.VMEM((n_mp, high, bs), BF16),
            pltpu.VMEM((bs, bs), BF16),
            pltpu.VMEM((bs, bs), F32),
            pltpu.VMEM((bs, bs), BF16),
            pltpu.VMEM((bs, bs), BF16),
            pltpu.VMEM((bs, bs), BF16),
            pltpu.VMEM((bs, bs), BF16),
            pltpu.VMEM((n_mp, high, bs), BF16),
            pltpu.VMEM((high, bs), BF16),
            pltpu.SemaphoreType.DMA((4,)),
            pltpu.SemaphoreType.DMA((2,)),
            pltpu.SemaphoreType.DMA((GROUPS,)),
            pltpu.SemaphoreType.DMA,
            pltpu.SemaphoreType.DMA((2,)),
            pltpu.SemaphoreType.DMA,
            pltpu.SemaphoreType.DMA,
            pltpu.SemaphoreType.DMA,
            pltpu.SemaphoreType.DMA,
            pltpu.SemaphoreType.DMA,
            pltpu.SemaphoreType.DMA,
            pltpu.SemaphoreType.REGULAR,
            pltpu.SemaphoreType.REGULAR((n_mp // row,)),
        ],
        compiler_params=pltpu.CompilerParams(collective_id=0, has_side_effects=True),
        name="refresh",
    )(plan, grads, factors.reshape(bs, bs), old)
    new_factor, fresh = pl.pallas_call(
        write_out,
        out_shape=(
            jax.ShapeDtypeStruct((bs, bs), F32),
            jax.ShapeDtypeStruct((n_mp, high, bs), BF16),
        ),
        in_specs=[pl.BlockSpec(memory_space=pl.ANY)] * 2,
        out_specs=(pl.BlockSpec(memory_space=pl.ANY),) * 2,
        scratch_shapes=[pltpu.SemaphoreType.DMA((2,))],
        compiler_params=pltpu.CompilerParams(vmem_limit_bytes=1 << 20),
        name="write_out",
    )(new_factor, fresh)
    return (new_factor[None, None], fresh.reshape(root_prev.shape))


def solution(mesh):
    return jax.shard_map(
        functools.partial(local, mesh.shape["dp"], mesh.shape["mp"]),
        mesh=mesh,
        in_specs=(
            P("dp", "mp", None, None, None),
            P("mp", "dp", None, None),
            P(None, "dp", "mp", None),
            P("dp", None),
        ),
        out_specs=(P("mp", "dp", None, None), P(None, "dp", "mp", None)),
        check_vma=False,
    )
```

```python
import functools

import jax
import jax.numpy as jnp
from jax import lax
from jax.experimental import pallas as pl
from jax.experimental.pallas import tpu as pltpu
from jax.sharding import PartitionSpec as P

keep_rate = 0.8
fresh_rate = 1.0 - keep_rate
GROUPS = 4
MESH = pl.DeviceIdType.MESH
F32 = jnp.float32
BF16 = jnp.bfloat16
scope = jax.named_scope


def mul(a, b, dims=(1, 0)):
    return lax.dot_general(a, b, (((dims[0],), (dims[1],)), ((), ())), preferred_element_type=F32)


def wait_bytes(ref, sem):
    pltpu.make_async_copy(ref, ref, sem).wait()


def kernel(
    n_dp, n_mp, blocks, row,
    plan, grad, fac, root, fresh, fac_out, plan_s,
    own_g, in_g, fac_v, pieces, full_x, rest, fifth, fac_b, summed, gram_b, out_v, detour,
    load_sem, grad_send, grad_recv, gram_send, gram_recv, root_send, root_recv, out_send, out_recv, detour_send, detour_recv, ready, above,
):
    d = lax.axis_index("dp")
    me = lax.axis_index("mp")
    bs = fac.shape[-1]
    high = bs // n_mp
    half = n_mp // 2
    hb = bs // 2
    wide = bs // GROUPS
    levels = n_mp // row
    level = me // row
    at = me % row
    band = row // 2
    upper_band = at >= band
    start = me - at % band
    side = me // half
    away = 1 - side
    near_cols = pl.ds(pl.multiple_of(side * hb, hb), hb)
    far_cols = pl.ds(pl.multiple_of(away * hb, hb), hb)
    far_first = pl.ds(pl.multiple_of(away * hb, hb), hb // 2)
    far_second = pl.ds(pl.multiple_of(away * hb + hb // 2, hb // 2), hb // 2)
    near_pieces = pl.ds(side * half, half)
    far_pieces = pl.ds(away * half, half)
    parity = me % 2
    collects = d % 2 == parity
    partner = d + 1 - 2 * (d % 2)

    loads = [
        pltpu.make_async_copy(root.at[me], pieces.at[me], load_sem.at[0]),
        pltpu.make_async_copy(fac, fac_v, load_sem.at[1]),
        pltpu.make_async_copy(plan, plan_s, load_sem.at[2]),
        pltpu.make_async_copy(grad.at[d // 2], own_g, load_sem.at[3]),
    ]

    def signal(sem, dp, mp):
        pl.semaphore_signal(sem, inc=1, device_id=(dp, mp), device_id_type=MESH)

    def strip(ref, c, by_cols):
        cut = pl.ds(c * wide, wide)
        return ref.at[:, cut] if by_cols else ref.at[cut, :]

    def strips(ref, c, by_cols):
        cut = pl.ds(c * wide, wide)
        return ref.at[:, :, cut] if by_cols else ref.at[:, cut, :]

    def by_parity(act):
        @pl.when(parity == 0)
        def _():
            act(True)

        @pl.when(parity == 1)
        def _():
            act(False)

    def send_grads(by_cols):
        for c in range(GROUPS):
            for k in range(blocks):
                to = 2 * k + parity

                @pl.when(to != d)
                def _():
                    pltpu.make_async_remote_copy(
                        src_ref=strip(grad.at[k], c, by_cols),
                        dst_ref=strip(in_g.at[(d - to + n_dp) % n_dp - 1], c, by_cols),
                        send_sem=grad_send.at[c // (GROUPS - 1)], recv_sem=grad_recv.at[c],
                        device_id=(to, me), device_id_type=MESH,
                    ).start()

    with scope("BARRIER"):
        barrier = pltpu.get_barrier_semaphore()
        odd_sender = jnp.logical_and(jnp.logical_not(collects), d % 2 == 1)

        @pl.when(collects)
        def _():
            for i in range(1, n_dp):
                signal(barrier, (d + i) % n_dp, me)

        @pl.when(odd_sender)
        def _():
            pl.semaphore_wait(barrier, blocks)
            send_grads(True)

        def greet(first):
            for i in range(band // 2):
                t = first + 2 * i + d % 2

                @pl.when(t != me)
                def _():
                    signal(barrier, d, t)

        for k in range(levels):
            @pl.when(level + k < levels)
            def _():
                greet(start + k * row)

                @pl.when(jnp.logical_not(upper_band))
                def _():
                    greet(start + k * row + band)

        @pl.when(collects)
        def _():
            loads[3].start()

        known = blocks - 1 + band - 1 + level * band + jnp.where(upper_band, (level + 1) * band, 0)

        @pl.when(jnp.logical_and(jnp.logical_not(collects), d % 2 == 0))
        def _():
            pl.semaphore_wait(barrier, blocks)
            send_grads(False)

        @pl.when(collects)
        def _():
            pl.semaphore_wait(barrier, known)
            if blocks > 1:
                by_parity(send_grads)
            signal(ready, d, me + 1 - 2 * parity)

        @pl.when(jnp.logical_and(upper_band, collects))
        def _():
            for k in range(levels):
                @pl.when(level >= k)
                def _():
                    pair = me - at % 2 - k * row
                    for i in range(2):
                        signal(above.at[k], d, pair - band + i)
                        if k:
                            signal(above.at[k], d, pair + i)

    def root_far(t):
        base = side * hb
        upper = me % half < half // 2

        def copy(start, size):
            cols = pl.ds(pl.multiple_of(start, hb // 2), size)
            pltpu.make_async_remote_copy(
                src_ref=root.at[t, :, cols], dst_ref=pieces.at[me, :, cols],
                send_sem=root_send, recv_sem=root_recv, device_id=(d, t), device_id_type=MESH,
            ).start()

        @pl.when(upper)
        def _():
            copy(base, hb)

        @pl.when(jnp.logical_not(upper))
        def _():
            copy(base + hb // 2, hb // 2)

    def root_near(t):
        pltpu.make_async_remote_copy(
            src_ref=root.at[t], dst_ref=pieces.at[me],
            send_sem=root_send, recv_sem=root_recv, device_id=(d, t), device_id_type=MESH,
        ).start()

    def send_roots(to, odd):
        for j in range(band // 2):
            t = to + (at // 2 * 2 + 2 * j) % band + odd
            close = t // half == side

            @pl.when(jnp.logical_not(close))
            def _():
                root_far(t)

            @pl.when(jnp.logical_and(close, t != me))
            def _():
                root_near(t)

    def each_level(odd, meet):
        for k in reversed(range(levels)):
            @pl.when(level >= k)
            def _():
                send_roots((level - k) * row, odd)

        if meet:
            @pl.when(jnp.logical_not(upper_band))
            def _():
                pl.semaphore_wait(above.at[0], 1)

        for k in reversed(range(levels)):
            @pl.when(level >= k)
            def _():
                send_roots((level - k) * row + band, odd)

        for k in range(1, levels):
            @pl.when(level + k < levels)
            def _():
                if meet:
                    pl.semaphore_wait(above.at[k], 1)
                send_roots((level + k) * row, odd)
                send_roots((level + k) * row + band, odd)

    with scope("ROOTSEND"):
        @pl.when(jnp.logical_not(collects))
        def _():
            pl.semaphore_wait(ready, 1)

        each_level(d % 2, True)
        for load in loads[:3]:
            load.start()

    def take(c, by_cols):
        wait_bytes(strips(in_g, c, by_cols), grad_recv.at[c])
        total = strip(own_g, c, by_cols)[...].astype(F32)
        for i in range(n_dp - 1):
            total += strip(in_g.at[i], c, by_cols)[...].astype(F32)
        strip(summed, c, by_cols)[...] = total.astype(BF16)

    def make_row(c, by_cols):
        new = strip(summed, c, by_cols)[...]
        so_far = pl.ds(0, (c + 1) * wide)
        product = mul(new, summed[:, so_far], (0, 0)) if by_cols else mul(new, summed[so_far, :], (1, 1))
        gram_b[pl.ds(c * wide, wide), so_far] = (fresh_rate * product).astype(BF16)

    def gram_row(c):
        part = gram_b.at[pl.ds(c * wide, wide), pl.ds(0, (c + 1) * wide)]
        return pltpu.make_async_remote_copy(
            src_ref=part, dst_ref=part, send_sem=gram_send, recv_sem=gram_recv.at[c // (GROUPS - 1)],
            device_id=(partner, me), device_id_type=MESH,
        )

    early = GROUPS // 2
    with scope("EARLY"):
        @pl.when(collects)
        def _():
            loads[3].wait()

            def act(by_cols):
                for c in range(early):
                    take(c, by_cols)
                    make_row(c, by_cols)
                    if c == 0:
                        each_level(1 - d % 2, False)

            by_parity(act)

        @pl.when(jnp.logical_not(collects))
        def _():
            wait_bytes(in_g.at[pl.ds(0, blocks), pl.ds(0, bs - wide), :], grad_send.at[0])
            each_level(1 - d % 2, False)

    with scope("ROOTRECV"):
        loads[0].wait()
        loads[1].wait()
        wait_bytes(pieces.at[pl.ds(0, half - 1 + half * 3 // 8)], root_recv)

    loads[2].wait()
    kept = plan_s[0, me] >= n_mp
    x_rate = jnp.where(kept, 1.0, 1.25)
    step = jnp.where(kept, 0.0, 0.25)

    with scope("ASSEMBLE"):
        near_rows = pieces[near_pieces].astype(F32).reshape(hb, bs).astype(BF16)
        full_x[near_cols, :] = near_rows
        full_x[far_cols, far_cols] = pieces[far_pieces, :, far_cols].astype(F32).reshape(hb, hb).astype(BF16)
        full_x[far_second, far_first] = full_x[far_first, far_second].astype(F32).T.astype(BF16)
        full_x[far_cols, near_cols] = full_x[near_cols, far_cols].astype(F32).T.astype(BF16)

    with scope("CHAIN"):
        x = full_x[...]
        square = mul(x, x).astype(BF16)
        fourth = mul(square, square).astype(BF16)
        fifth[...] = (step * mul(x, fourth)).astype(BF16)

    def send_out(t):
        pltpu.make_async_remote_copy(
            src_ref=out_v.at[t], dst_ref=fresh.at[me],
            send_sem=out_send, recv_sem=out_recv, device_id=(d, t), device_id_type=MESH,
        ).start()

    middle = levels // 2
    even = d % 2 == 0
    hands = jnp.logical_and(jnp.logical_and(collects, even), level == middle)
    helps = jnp.logical_not(jnp.logical_or(collects, even))
    first_hop = jnp.logical_and(helps, level == middle)
    second_hop = jnp.logical_and(helps, level == middle - 1)

    def send_far(t):
        aside = jnp.logical_and(hands, t == me - row)

        @pl.when(aside)
        def _():
            pltpu.make_async_remote_copy(
                src_ref=out_v.at[t], dst_ref=detour,
                send_sem=out_send, recv_sem=detour_recv, device_id=(partner, me), device_id_type=MESH,
            ).start()

        @pl.when(jnp.logical_not(aside))
        def _():
            send_out(t)

    def hand_on(to, dst, sem):
        wait_bytes(detour, detour_recv)
        pltpu.make_async_remote_copy(
            src_ref=detour, dst_ref=dst,
            send_sem=detour_send, recv_sem=sem, device_id=to, device_id_type=MESH,
        ).start()

    def refine(first, count, value):
        rows = pl.ds(pl.multiple_of(first * high, high), count * high)
        out_v[pl.ds(first, count)] = value(rows).reshape(count, high, bs).astype(BF16)

    def give_far(k, value):
        to = away * half + k * row
        refine(to, row, value)
        for j in range(row):
            turn = jnp.where(to == 0, j // band, (j // band + 1 + upper_band.astype(jnp.int32)) % 2)
            send_far(to + turn * band + (j + d) % band)

    def give_near(value):
        refine(side * half, half, value)

        @pl.loop(1, half)
        def _(i):
            send_out(side * half + (me + i) % half)

    def with_factor(rows):
        return x_rate * full_x[rows, :].astype(F32) - mul(fifth[rows, :], fac_b[...])

    @pl.when(collects)
    def _():
        def act(by_cols):
            dims = (1, 1) if by_cols else (0, 0)
            across = (1, 0) if by_cols else (1, 1)
            back = (1, 1) if by_cols else (1, 0)
            last = GROUPS - 1
            first_rows = pl.ds(pl.multiple_of(away * hb, hb), row * high)
            if by_cols:
                with scope("GRADS"):
                    for c in range(early, last):
                        take(c, by_cols)
                        make_row(c, by_cols)
                    for c in range(last):
                        gram_row(c).start()
                    known = summed[:, pl.ds(0, last * wide)]
                    total = keep_rate * fac_v[...] + fresh_rate * mul(known, known, dims)
                    fac_out[...] = total
                    fac_b[...] = total.astype(BF16)
                    rest[first_rows, :] = with_factor(first_rows)
                with scope("GRADLAST"):
                    take(last, by_cols)
                    new = strip(summed, last, by_cols)[...]
                    turned = (fresh_rate * mul(fifth[first_rows, :], new, across)).astype(BF16)
                    give_far(0, lambda rows: rest[rows, :] - mul(turned, new, back))
                with scope("ROWLAST"):
                    make_row(last, by_cols)
                    gram_row(last).start()
                with scope("GIVEFAR"):
                    fac_b[...] = (fac_out[...] + fresh_rate * mul(new, new, dims)).astype(BF16)
            else:
                with scope("GRADS"):
                    for c in range(early):
                        gram_row(c).start()
                    for c in range(early, GROUPS):
                        take(c, by_cols)
                    whole = summed[...]
                    total = keep_rate * fac_v[...] + fresh_rate * mul(whole, whole, dims)
                    fac_out[...] = total
                    fac_b[...] = total.astype(BF16)
                with scope("GRADLAST"):
                    give_far(0, with_factor)
                with scope("ROWLAST"):
                    for c in range(early, GROUPS):
                        make_row(c, by_cols)
                        gram_row(c).start()
            with scope("GIVEFAR"):
                for k in range(1, half // row):
                    give_far(k, with_factor)
            with scope("GIVENEAR"):
                give_near(with_factor)
            if by_cols:
                with scope("FACOUT"):
                    fac_out[...] += fresh_rate * mul(new, new, dims)
            wait_bytes(gram_b.at[pl.ds(0, bs * (GROUPS + 1) // (2 * GROUPS))], gram_send)

        by_parity(act)

    @pl.when(jnp.logical_not(collects))
    def _():
        with scope("REST"):
            rest[...] = x_rate * full_x[...].astype(F32) - keep_rate * mul(fifth[...], fac_v[...].astype(BF16))
        def mirror(c):
            rows = pl.ds(c * wide, wide)
            before = pl.ds(0, c * wide)
            gram_b[before, rows] = gram_b[rows, before].astype(F32).T.astype(BF16)

        last = GROUPS - 1
        with scope("GRAMIN"):
            wait_bytes(gram_b.at[pl.ds(0, last * wide), pl.ds(0, bs // 2)], gram_recv.at[0])
            for c in range(1, last):
                mirror(c)

            @pl.when(first_hop)
            def _():
                hand_on((d, me - row), detour, detour_recv)
        with scope("GRAMLAST"):
            gram_row(last).wait_recv()
            mirror(last)

        def with_gram(rows):
            return rest[rows, :] - mul(fifth[rows, :], gram_b[...])

        with scope("GIVEFAR"):
            for k in range(half // row):
                give_far(k, with_gram)
        with scope("GIVENEAR"):
            give_near(with_gram)
        with scope("FACOUT"):
            fac_out[...] = keep_rate * fac_v[...] + gram_b[...].astype(F32)
            wait_bytes(in_g.at[pl.ds(0, blocks), pl.ds(0, wide), :], grad_send.at[1])

            @pl.when(second_hop)
            def _():
                hand_on((partner, me), fresh.at[me + row], out_recv)

            @pl.when(jnp.logical_or(first_hop, second_hop))
            def _():
                wait_bytes(detour, detour_send)

    with scope("SENDS"):
        own_out = pltpu.make_async_copy(out_v.at[me], fresh.at[me], load_sem.at[0])
        own_out.start()
        if blocks > 1:
            @pl.when(collects)
            def _():
                wait_bytes(in_g.at[pl.ds(0, blocks - 1), pl.ds(0, bs - wide), :], grad_send.at[0])
                wait_bytes(in_g.at[pl.ds(0, blocks - 1), pl.ds(0, wide), :], grad_send.at[1])

        @pl.when(me % half < half // 2)
        def _():
            wait_bytes(pieces.at[pl.ds(0, half - 1 + half // 2)], root_send)

        @pl.when(me % half >= half // 2)
        def _():
            wait_bytes(pieces.at[pl.ds(0, half - 1 + half // 4)], root_send)

        own_out.wait()
        wait_bytes(out_v.at[pl.ds(0, n_mp - 1)], out_send)

    with scope("RECV"):
        wait_bytes(fresh.at[pl.ds(0, n_mp - 1)], out_recv)


def write_out(fac_v, fresh_v, fac_out, fresh_out, sem):
    copies = [
        pltpu.make_async_copy(fac_v, fac_out, sem.at[0]),
        pltpu.make_async_copy(fresh_v, fresh_out, sem.at[1]),
    ]
    for copy in copies:
        copy.start()
    for copy in copies:
        copy.wait()


def level_size(n_mp):
    size = 1
    while size * size < n_mp:
        size *= 2
    return size


def local(n_dp, n_mp, grad_parts, factors, root_prev, plan):
    blocks, bs = grad_parts.shape[2], factors.shape[-1]
    high = bs // n_mp
    row = level_size(n_mp)
    wide = bs // GROUPS
    grads = grad_parts.reshape(blocks, bs, bs)
    old = root_prev.reshape(n_mp, high, bs)
    fresh, new_factor = pl.pallas_call(
        functools.partial(kernel, n_dp, n_mp, blocks, row),
        out_shape=(
            pltpu.VMEM((n_mp, high, bs), BF16),
            pltpu.VMEM((bs, bs), F32),
        ),
        in_specs=[pl.BlockSpec(memory_space=pl.ANY)] * 4,
        out_specs=(pl.BlockSpec(memory_space=pltpu.VMEM),) * 2,
        scratch_shapes=[
            pltpu.SMEM(plan.shape, plan.dtype),
            pltpu.VMEM((bs, bs), BF16),
            pltpu.VMEM((n_dp - 1, bs, bs), BF16),
            pltpu.VMEM((bs, bs), F32),
            pltpu.VMEM((n_mp, high, bs), BF16),
            pltpu.VMEM((bs, bs), BF16),
            pltpu.VMEM((bs, bs), F32),
            pltpu.VMEM((bs, bs), BF16),
            pltpu.VMEM((bs, bs), BF16),
            pltpu.VMEM((bs, bs), BF16),
            pltpu.VMEM((bs, bs), BF16),
            pltpu.VMEM((n_mp, high, bs), BF16),
            pltpu.VMEM((high, bs), BF16),
            pltpu.SemaphoreType.DMA((4,)),
            pltpu.SemaphoreType.DMA((2,)),
            pltpu.SemaphoreType.DMA((GROUPS,)),
            pltpu.SemaphoreType.DMA,
            pltpu.SemaphoreType.DMA((2,)),
            pltpu.SemaphoreType.DMA,
            pltpu.SemaphoreType.DMA,
            pltpu.SemaphoreType.DMA,
            pltpu.SemaphoreType.DMA,
            pltpu.SemaphoreType.DMA,
            pltpu.SemaphoreType.DMA,
            pltpu.SemaphoreType.REGULAR,
            pltpu.SemaphoreType.REGULAR((n_mp // row,)),
        ],
        compiler_params=pltpu.CompilerParams(collective_id=0, has_side_effects=True),
        name="refresh",
    )(plan, grads, factors.reshape(bs, bs), old)
    new_factor, fresh = pl.pallas_call(
        write_out,
        out_shape=(
            jax.ShapeDtypeStruct((bs, bs), F32),
            jax.ShapeDtypeStruct((n_mp, high, bs), BF16),
        ),
        in_specs=[pl.BlockSpec(memory_space=pl.ANY)] * 2,
        out_specs=(pl.BlockSpec(memory_space=pl.ANY),) * 2,
        scratch_shapes=[pltpu.SemaphoreType.DMA((2,))],
        compiler_params=pltpu.CompilerParams(vmem_limit_bytes=1 << 20),
        name="write_out",
    )(new_factor, fresh)
    return (new_factor[None, None], fresh.reshape(root_prev.shape))


def solution(mesh):
    return jax.shard_map(
        functools.partial(local, mesh.shape["dp"], mesh.shape["mp"]),
        mesh=mesh,
        in_specs=(
            P("dp", "mp", None, None, None),
            P("mp", "dp", None, None),
            P(None, "dp", "mp", None),
            P("dp", None),
        ),
        out_specs=(P("mp", "dp", None, None), P(None, "dp", "mp", None)),
        check_vma=False,
    )
```
